128 devices in a mesh: row: 16 (over z_hi, y, core), col: 8 (over x, z_lo).
Axes of the slice: x: 4, y: 4, z: 4 (z_hi: 2, z_lo: 2; z = z_hi * 2 + z_lo), core: 2. Of those that a mesh axis runs over, the one named last changes fastest.
Arguments:
- observed: float32 [2048, 4096], P('row', 'col'), may hold values from -6 to 6
- psf_table: bfloat16 [64, 31, 31], replicated, may hold values from 0.049804688 to 1
- psf_index: int32 [16, 32], P('row', 'col'), may hold values from 0 to 63
- start_image: float32 [2048, 4096], P('row', 'col'), may hold values from -6 to 6
- blur_dual: float32 [2048, 4096], P('row', 'col'), may hold values from -6 to 6
- tv_dual: float32 [2, 2048, 4096], P(None, 'row', 'col'), may hold values from -1.8 to 1.8
Outputs:
- restored: float32 [2048, 4096], P('row', 'col')
- blur_dual_out: float32 [2048, 4096], P('row', 'col')
The draws below stay inside these ranges and needn't reach their ends.
Inputs may be any that keep to these rules, and one draw needn't show every extreme that they name: `psf_index`: each entry names a row of psf_table.
All inputs are finite; a program needn't handle non-finite values.
Results may differ from the reference program's by a relative error of at most 0.0003.
Values may be sent and summed in bfloat16 or wider, within the bound.
A program may use at most 128 MiB of HBM per device.

```python
import math
import jax
import jax.numpy as jnp
from jax import lax

KS = 31
PR = 128
PC = 128
NPSF = 64
ITERS = 2
NX = 2048
NY = 4096
NPC = 32
N_ROW = 16


def plant(values, own_key, low, high):
    spot = [jax.random.randint(jax.random.fold_in(own_key, axis), (), 0, length) for axis, length in enumerate(values.shape)]
    widest = values.shape.index(max(values.shape))
    neighbour = spot[:widest] + [(spot[widest] + 1) % values.shape[widest]] + spot[widest + 1:]
    return values.at[tuple(spot)].set(low).at[tuple(neighbour)].set(high)


def steps_of(own_key, extent, split, low, largest):
    level = 1.0
    for position, parts in split:
        steps = jax.random.uniform(jax.random.fold_in(jax.random.fold_in(own_key, 6), position), (parts,), jnp.float32, low / len(split), largest / len(split))
        level = level * jnp.repeat(jnp.exp(steps), extent[position] // parts).reshape((-1,) + (1,) * (len(extent) - 1 - position))
    return level


def noise(rng, shape, scale, limit, split=(), kind=jnp.bfloat16):
    factor_of = steps_of(rng, shape, split, -0.22, 0.18) if split else 1.0
    array = jax.random.normal(rng, shape, jnp.float32) * scale * factor_of
    return jnp.minimum(jnp.maximum(array, -limit), limit).astype(kind)


def setup_inputs(seed: int = 0) -> dict:
    key_of = jax.random.split(jax.random.key(seed), 7)
    observed = noise(key_of[0], (NX, NY), 1.0, 6.0, ((0, 16), (1, 8)), jnp.float32)
    psf_table = jnp.clip(jnp.exp(jax.random.uniform(key_of[1], (NPSF, KS, KS), jnp.float32, math.log(0.049804688), math.log(1.0))), 0.049804688, 1.0).astype(jnp.bfloat16)
    psf_index = plant(jax.random.randint(key_of[2], (N_ROW, NPC), 0, NPSF), jax.random.fold_in(key_of[2], 1), 0, NPSF - 1).astype(jnp.int32)
    start_image = noise(key_of[3], (NX, NY), 1.0, 6.0, ((0, 16), (1, 8)), jnp.float32)
    blur_dual = noise(key_of[4], (NX, NY), 1.0, 6.0, ((0, 16), (1, 8)), jnp.float32)
    tv_dual = noise(key_of[5], (2, NX, NY), 0.3, 1.8, ((1, 16), (2, 8)), jnp.float32)
    return {"observed": observed, "psf_table": psf_table, "psf_index": psf_index, "start_image": start_image, "blur_dual": blur_dual, "tv_dual": tv_dual}


sigma_step = 0.15
tau_step = 0.6
tv_weight = 0.5
group_size = 4

def make_select(kernel_size, patch_cols):
    half_width = kernel_size // 2
    column_in = jnp.arange(patch_cols + 2 * half_width, dtype=jnp.int32)[None, :, None]
    column_out = jnp.arange(patch_cols, dtype=jnp.int32)[None, None, :]
    tap_index = jnp.arange(kernel_size, dtype=jnp.int32)[:, None, None]
    return (column_in - column_out == tap_index).astype(jnp.float32)

def strip_pass(strip_in, observed_s, dual_s, index_s, kern_flat, select):
    kernel_size = select.shape[0]
    patch_cols = select.shape[2]
    half_width = (select.shape[1] - patch_cols) // 2
    patch_rows, width = observed_s.shape
    group_span = group_size * patch_cols
    group_count = width // group_span
    table_size = kern_flat.shape[0]

    def one_group(spread_sum, group_id):
        first_col = group_id * group_span
        window = lax.dynamic_slice_in_dim(strip_in, first_col, group_span + 2 * half_width, 1)
        pieces = jnp.stack([window[:, member * patch_cols:member * patch_cols + patch_cols + 2 * half_width] for member in range(group_size)])
        stacked = jnp.stack([pieces[:, tap_row:tap_row + patch_rows, :] for tap_row in range(kernel_size)], axis=2)
        patch_ids = lax.dynamic_slice_in_dim(index_s, group_id * group_size, group_size)
        onehot = (patch_ids[:, None] == jnp.arange(table_size, dtype=jnp.int32)[None, :]).astype(jnp.float32)
        kernels = jnp.dot(onehot, kern_flat, precision=lax.Precision.HIGHEST).reshape(group_size, kernel_size, kernel_size)
        toeplitz = jnp.einsum('pab,bkj->pakj', kernels, select, precision=lax.Precision.HIGHEST)
        blurred = jnp.einsum('piak,pakj->pij', stacked, toeplitz, precision=lax.Precision.HIGHEST)
        blurred = blurred.transpose(1, 0, 2).reshape(patch_rows, group_span)
        seen_group = lax.dynamic_slice_in_dim(observed_s, first_col, group_span, 1)
        dual_group = lax.dynamic_slice_in_dim(dual_s, first_col, group_span, 1)
        dual_new = (dual_group + sigma_step * (blurred - seen_group)) / (1.0 + sigma_step)
        rounded = lax.optimization_barrier(dual_new.astype(jnp.bfloat16)).astype(jnp.float32)
        rounded = rounded.reshape(patch_rows, group_size, patch_cols).transpose(1, 0, 2)
        padded_dual = jnp.pad(rounded, ((0, 0), (kernel_size - 1, kernel_size - 1), (0, 0)))
        shifted = jnp.stack([padded_dual[:, kernel_size - 1 - tap_row:kernel_size - 1 - tap_row + patch_rows + 2 * half_width, :] for tap_row in range(kernel_size)], axis=2)
        spread = jnp.einsum('praj,pakj->prk', shifted, toeplitz, precision=lax.Precision.HIGHEST)
        merged = jnp.zeros((patch_rows + 2 * half_width, group_span + 2 * half_width), jnp.float32)
        for member in range(group_size):
            merged = merged.at[:, member * patch_cols:member * patch_cols + patch_cols + 2 * half_width].add(spread[member])
        previous = lax.dynamic_slice_in_dim(spread_sum, first_col, group_span + 2 * half_width, 1)
        spread_sum = lax.dynamic_update_slice_in_dim(spread_sum, previous + merged, first_col, 1)
        return (spread_sum, dual_new)
    start_sum = jnp.zeros((patch_rows + 2 * half_width, width + 2 * half_width), jnp.float32)
    spread_sum, duals = lax.scan(one_group, start_sum, jnp.arange(group_count, dtype=jnp.int32))
    return (duals.transpose(1, 0, 2).reshape(patch_rows, width), spread_sum)

def reference(observed, psf_table, psf_index, start_image, blur_dual, tv_dual):
    half_width = KS // 2
    table = psf_table.astype(jnp.float32)
    normed = table / lax.optimization_barrier(jnp.sum(table, axis=(1, 2), keepdims=True))
    kern_flat = lax.optimization_barrier(normed.astype(jnp.bfloat16)).astype(jnp.float32).reshape(NPSF, KS * KS)
    select = make_select(KS, PC)
    restored = start_image
    extrapolated = start_image
    dual_now = blur_dual
    tv_rows = tv_dual[0]
    tv_cols = tv_dual[1]
    keep_rows = (jnp.arange(NX, dtype=jnp.int32) < NX - 1)[:, None]
    keep_cols = (jnp.arange(NY, dtype=jnp.int32) < NY - 1)[None, :]
    for step in range(ITERS):
        padded = lax.optimization_barrier(jnp.pad(extrapolated, half_width).astype(jnp.bfloat16)).astype(jnp.float32)

        def one_strip(carry, strip_id):
            start_row = strip_id * PR
            strip_in = lax.dynamic_slice_in_dim(padded, start_row, PR + 2 * half_width, 0)
            seen_strip = lax.dynamic_slice_in_dim(observed, start_row, PR, 0)
            dual_strip = lax.dynamic_slice_in_dim(dual_now, start_row, PR, 0)
            index_strip = lax.dynamic_index_in_dim(psf_index, strip_id, 0, keepdims=False)
            new_dual, spread_sum = strip_pass(strip_in, seen_strip, dual_strip, index_strip, kern_flat, select)
            return (carry, (new_dual, spread_sum))
        unused, (dual_strips, spread_strips) = lax.scan(one_strip, jnp.zeros((), jnp.float32), jnp.arange(N_ROW, dtype=jnp.int32))
        dual_now = dual_strips.reshape(NX, NY)

        def add_strip(strip_id, total):
            piece = spread_strips[strip_id]
            start_row = (strip_id * PR).astype(jnp.int32)
            zero_col = jnp.zeros((), jnp.int32)
            previous = lax.dynamic_slice(total, (start_row, zero_col), piece.shape)
            return lax.dynamic_update_slice(total, previous + piece, (start_row, zero_col))
        total = lax.fori_loop(0, N_ROW, add_strip, jnp.zeros((NX + 2 * half_width, NY + 2 * half_width), jnp.float32))
        adjoint = total[half_width:half_width + NX, half_width:half_width + NY]
        below = jnp.concatenate([extrapolated[1:], jnp.zeros((1, NY), jnp.float32)], axis=0)
        right = jnp.concatenate([extrapolated[:, 1:], jnp.zeros((NX, 1), jnp.float32)], axis=1)
        grad_rows = jnp.where(keep_rows, below - extrapolated, 0.0)
        grad_cols = jnp.where(keep_cols, right - extrapolated, 0.0)
        moved_rows = tv_rows + sigma_step * grad_rows
        moved_cols = tv_cols + sigma_step * grad_cols
        shrink = jnp.maximum(1.0, jnp.sqrt(moved_rows * moved_rows + moved_cols * moved_cols) / tv_weight)
        tv_rows = moved_rows / shrink
        tv_cols = moved_cols / shrink
        masked_rows = jnp.where(keep_rows, tv_rows, 0.0)
        masked_cols = jnp.where(keep_cols, tv_cols, 0.0)
        diverge = masked_rows - jnp.concatenate([jnp.zeros((1, NY), jnp.float32), masked_rows[:-1]], axis=0)
        diverge = diverge + masked_cols - jnp.concatenate([jnp.zeros((NX, 1), jnp.float32), masked_cols[:, :-1]], axis=1)
        next_image = restored - tau_step * (adjoint - diverge)
        extrapolated = 2.0 * next_image - restored
        restored = next_image
    return (restored, dual_now)
```

```python
import jax
import jax.numpy as jnp
from jax import lax
from jax.experimental import pallas as pl
from jax.experimental.pallas import tpu as pltpu
from jax.sharding import PartitionSpec as P

ITERS = 2
SIGMA = 0.15
TAU = 0.6
WEIGHT = 0.5
TAPS = 31
PAIRS = 64
TILES = 4
DIRS = ((-1, 0), (1, 0), (0, -1), (0, 1), (-1, -1), (-1, 1), (1, -1), (1, 1))
MESH_ID = pl.DeviceIdType.MESH
F32 = jnp.float32
BF16 = jnp.bfloat16


def lanes(shape):
    return lax.broadcasted_iota(jnp.int32, shape, 1)


def roll(value, shift):
    shift = shift % 128
    return value if shift == 0 else pltpu.roll(value, shift, 1)


def kernel(
    index_ref, observed_hbm, table_hbm, start_hbm, dual_hbm, tv_hbm,
    restored_hbm, dual_out_hbm,
    start_v, table_v, observed_v, dual_v, tv_v, out_v,
    kern_v, base_v, weights, x_v, bar_v, obs_v, y_v, q1_v, q2_v, shifted, ypad, spread, acc,
    row_out, col_out, cor_out, row_in, col_in, cor_in,
    load_sem, store_sem, send_sem, recv_sem,
):
    row, col = lax.axis_index("row"), lax.axis_index("col")
    rows, cols = lax.axis_size("row"), lax.axis_size("col")

    def at(direction):
        dr, dc = direction
        return (lax.rem(row + dr + rows, rows), lax.rem(col + dc + cols, cols))

    barrier = pltpu.get_barrier_semaphore()
    for direction in DIRS:
        pl.semaphore_signal(barrier, inc=1, device_id=at(direction), device_id_type=MESH_ID)

    slices = [slice(128 * p, 128 * p + 128) for p in range(TILES)]
    plain = ((start_hbm, start_v), (observed_hbm, observed_v), (dual_hbm, dual_v))
    sources = [(src.at[:, slices[p]], dst.at[p]) for src, dst in plain for p in range(TILES)]
    sources += [(tv_hbm.at[:, :, slices[p]], tv_v.at[:, p]) for p in range(TILES)]
    sources.insert(TILES, (table_hbm, table_v))
    loads = [pltpu.make_async_copy(src, dst, load_sem.at[i]) for i, (src, dst) in enumerate(sources)]
    for load in loads:
        load.start()

    top, bottom = row == 0, row == rows - 1
    left, right = col == 0, col == cols - 1
    outside = (top, bottom, left, right, top | left, top | right, bottom | left, bottom | right)
    lane64 = lanes((PAIRS, 128))
    lane8 = lanes((8, 128))
    lane16 = lanes((16, 128))
    sub64 = lax.broadcasted_iota(jnp.int32, (PAIRS, 128), 0)

    def copies(exchange):
        result = []
        for d, direction in enumerate(DIRS):
            if d < 2:
                src, dst = row_out.at[exchange, d], row_in.at[exchange, d ^ 1]
            elif d < 4:
                src, dst = col_out.at[exchange, d - 2], col_in.at[exchange, (d - 2) ^ 1]
            else:
                src, dst = cor_out.at[exchange, d - 4], cor_in.at[exchange, 3 - (d - 4)]
            back = d ^ 1 if d < 4 else 4 + 3 - (d - 4)
            result.append(
                pltpu.make_async_remote_copy(
                    src_ref=src,
                    dst_ref=dst,
                    send_sem=send_sem.at[exchange, d],
                    recv_sem=recv_sem.at[exchange, back],
                    device_id=at(direction),
                    device_id_type=MESH_ID,
                )
            )
        return result

    def wait_in(exchange):
        for copy in copies(exchange):
            copy.wait()

    def packed(parts, first_lane, height):
        lane = lane16 if height == 16 else lane8
        message = None
        for f, part in enumerate(parts):
            moved = roll(part, 16 * f - first_lane)
            message = moved if f == 0 else jnp.where(lane >= 16 * f, moved, message)
        return message

    def unpacked(message, f, first_lane):
        return roll(message, first_lane - 16 * f)

    for load in loads[:TILES]:
        load.wait()
    for par in (0, 1):
        for p in range(TILES):
            value = start_v[p, pl.ds(par, PAIRS, stride=2), :]
            x_v[par, p] = value
            bar_v[par, p] = value

    def send_image(exchange):
        for d, first in ((0, 0), (1, PAIRS - 8)):
            for par in (0, 1):
                for p in range(TILES):
                    row_out[exchange, d, par, p] = bar_v[par, p, first : first + 8]
        for s, (p, first_lane) in enumerate(((0, 0), (TILES - 1, 112))):
            col_out[exchange, s] = packed(
                [bar_v[par, p, 16 * k : 16 * k + 16] for par in (0, 1) for k in range(4)], first_lane, 16
            )
            for d, first in ((0, 0), (1, PAIRS - 8)):
                cor_out[exchange, 2 * d + s] = packed(
                    [bar_v[par, p, first : first + 8] for par in (0, 1)], first_lane, 8
                )
        for copy in copies(exchange):
            copy.start()

    pl.semaphore_wait(barrier, len(DIRS))
    send_image(0)

    kern_v[...] = jnp.zeros_like(kern_v)
    loads[TILES].wait()
    for p in range(TILES):
        table = table_v[index_ref[0, p]].astype(F32)
        kern_v[8 + 32 * p : 8 + 32 * p + TAPS, 0:TAPS] = table / jnp.sum(table)
    tap = lax.broadcasted_iota(jnp.int32, (128, 128), 0)
    place = lanes((128, 128))
    flip_low = ((tap < TAPS) & (place == lax.rem(128 - tap, 128))).astype(F32).astype(BF16)
    flip_high = ((tap < TAPS) & (place == 64 - tap)).astype(F32).astype(BF16)
    base_v[...] = jnp.dot(kern_v[8:136].astype(BF16), flip_low, preferred_element_type=F32) + jnp.dot(
        kern_v[7:135].astype(BF16), flip_high, preferred_element_type=F32
    )
    reach = tap - (place & 63)
    band = (reach >= 0) & (reach < TAPS)

    unroll = 4

    def build(step, carry):
        for u in range(unroll):
            r = step * unroll + u
            line = jnp.broadcast_to(base_v[pl.ds(r, 1), :], (128, 128))
            rolled = pltpu.roll(line, 0, 1, stride=1, stride_axis=0)
            weights[pl.ds(pl.multiple_of(r * 128, 128), 128), :] = jnp.where(band, rolled, 0.0).astype(BF16)
        return carry

    lax.fori_loop(0, 128 // unroll, build, 0)

    ypad[...] = jnp.zeros_like(ypad)
    for load in loads[TILES + 1 :]:
        load.wait()
    for par in (0, 1):
        for p in range(TILES):
            rows_of = pl.ds(par, PAIRS, stride=2)
            obs_v[par, p] = observed_v[p, rows_of, :]
            y_v[par, p] = dual_v[p, rows_of, :]
            q1_v[par, p] = tv_v[0, p, rows_of, :]
            q2_v[par, p] = tv_v[1, p, rows_of, :]

    for step in range(ITERS):
        halo, fold = 2 * step, 2 * step + 1
        wait_in(halo)
        rows_in = [
            [
                [jnp.where(outside[d], 0.0, row_in[halo, d, par, p]) for p in range(TILES)]
                for par in (0, 1)
            ]
            for d in (0, 1)
        ]
        cols_in = [jnp.where(outside[2 + s], 0.0, col_in[halo, s]) for s in (0, 1)]
        cors_in = [jnp.where(outside[4 + s], 0.0, cor_in[halo, s]) for s in range(4)]

        def sides(par, first_lanes):
            return [
                jnp.concatenate(
                    [unpacked(cols_in[s], 4 * par + k, first_lanes[s]) for k in range(4)], axis=0
                )
                for s in (0, 1)
            ]

        def lay(tiles, par, first, count):
            lane = lanes((count, 128))
            by15 = [roll(t, 15) for t in tiles[:-1]]
            by79 = [roll(t, 79) for t in tiles[1:]]
            for p in range(TILES):
                shifted[par, 0, p, first : first + count] = jnp.where(lane < 15, by15[p], by15[p + 1])
                shifted[par, 1, p, first : first + count] = jnp.where(lane < 79, by79[p], by79[p + 1])

        side_tiles = [sides(par, (112, 0)) for par in (0, 1)]
        for par in (0, 1):
            lay(
                [side_tiles[par][0]] + [bar_v[par, p] for p in range(TILES)] + [side_tiles[par][1]], par, 8, PAIRS
            )
            for d, first in ((0, 0), (1, 72)):
                lay(
                    [unpacked(cors_in[2 * d], par, 112)]
                    + rows_in[d][par]
                    + [unpacked(cors_in[2 * d + 1], par, 0)],
                    par,
                    first,
                    8,
                )

        def blur(p, carry):
            pieces = []
            for t in range(16):
                pieces.append(
                    jnp.concatenate([shifted[0 + 1, h, p, t : t + PAIRS] for h in (0, 1)], axis=0).astype(BF16)
                )
                pieces.append(
                    jnp.concatenate([shifted[0, h, p, t + 1 : t + 1 + PAIRS] for h in (0, 1)], axis=0).astype(BF16)
                )
            stacked = jnp.concatenate(pieces, axis=1)
            matrix = weights[pl.ds(pl.multiple_of(p * 4096, 4096), 4096), :]
            blurred = jnp.dot(stacked, matrix, preferred_element_type=F32)
            first, second = blurred[:PAIRS], blurred[PAIRS:]
            even = jnp.where(lane64 < 64, first, roll(second, 64))
            odd = jnp.where(lane64 < 64, roll(first, 64), second)
            new = []
            for par, value in ((0, even), (1, odd)):
                updated = (y_v[par, p] + SIGMA * (value - obs_v[par, p])) / (1.0 + SIGMA)
                y_v[par, p] = updated
                new.append(updated)
            ypad[0, p, 16 : 16 + PAIRS] = jnp.where(lane64 < 64, new[0], roll(new[1], 64))
            ypad[1, p, 16 : 16 + PAIRS] = jnp.where(lane64 < 64, roll(new[0], 64), new[1])
            return carry

        lax.fori_loop(0, TILES, blur, 0)

        for p in range(TILES):
            even, odd = bar_v[0, p], bar_v[1, p]
            below = jnp.concatenate([even[1:], rows_in[1][0][p][:1]], axis=0)
            grad_even = odd - even
            grad_odd = jnp.where((sub64 == PAIRS - 1) & bottom, 0.0, below - odd)
            for par, value, grad1 in ((0, even, grad_even), (1, odd, grad_odd)):
                beyond = bar_v[par, p + 1] if p + 1 < TILES else side_tiles[par][1]
                after = jnp.where(lane64 < 127, roll(value, 127), roll(beyond, 127))
                grad2 = after - value
                if p + 1 == TILES:
                    grad2 = jnp.where((lane64 == 127) & right, 0.0, grad2)
                u1 = q1_v[par, p] + SIGMA * grad1
                u2 = q2_v[par, p] + SIGMA * grad2
                shrink = jnp.maximum(1.0, jnp.sqrt(u1 * u1 + u2 * u2) / WEIGHT)
                q1_v[par, p] = u1 / shrink
                q2_v[par, p] = u2 / shrink

        def adjoint(p, carry):
            pieces = [
                jnp.concatenate([ypad[h, p, 16 - t : 96 - t] for h in (0, 1)], axis=0).astype(BF16)
                for t in range(16)
            ]
            stacked = jnp.concatenate(pieces, axis=1)
            start = pl.multiple_of(p * 4096, 4096)
            matrix = jnp.concatenate(
                [weights[pl.ds(start + 256 * t, 256), :] for t in range(16)], axis=1
            )
            out = lax.dot_general(stacked, matrix, (((1,), (1,)), ((), ())), preferred_element_type=F32)
            for h in (0, 1):
                spread[1, h, p, 0:80] = out[80 * h : 80 * h + 80, 0:128]
                spread[0, h, p, 1:81] = out[80 * h : 80 * h + 80, 128:256]
            return carry

        lax.fori_loop(0, TILES, adjoint, 0)
        lane80 = lanes((80, 128))
        sub80 = lax.broadcasted_iota(jnp.int32, (80, 128), 0)
        for par in (0, 1):
            halves = [roll(spread[par, 1, p, 0:80], 64) for p in range(TILES)]
            total = []
            for q in range(TILES + 1):
                if q == 0:
                    value = spread[par, 0, 0, 0:80] + jnp.where(lane80 >= 64, halves[0], 0.0)
                elif q == TILES:
                    value = jnp.where(lane80 < 64, halves[q - 1], 0.0)
                else:
                    value = spread[par, 0, q, 0:80] + jnp.where(lane80 >= 64, halves[q], halves[q - 1])
                if par == 0:
                    value = jnp.where(sub80 == 0, 0.0, value)
                total.append(roll(value, 113))
            acc[par, 0] = jnp.where(lane80 >= 113, total[0], 0.0)
            for p in range(TILES):
                acc[par, p + 1] = jnp.where(lane80 < 113, total[p], total[p + 1])
            last = jnp.where(lane80 < 15, total[TILES], 0.0)
            acc[par, TILES + 1] = last
            acc[par, TILES + 1, 8:72] = last[8:72] + jnp.where(lane64 == 0, roll(q2_v[par, TILES - 1], 1), 0.0)

        for p in range(TILES):
            edge = jnp.concatenate([q1_v[1, p, PAIRS - 1 : PAIRS], jnp.zeros((7, 128), F32)], axis=0)
            acc[0, p + 1, 72:80] = acc[0, p + 1, 72:80] + edge
        for d, first in ((0, 0), (1, 72)):
            for par in (0, 1):
                for p in range(TILES):
                    row_out[fold, d, par, p] = acc[par, p + 1, first : first + 8]
        for s, (q, first_lane) in enumerate(((0, 112), (TILES + 1, 0))):
            col_out[fold, s] = packed(
                [acc[par, q, 8 + 16 * k : 24 + 16 * k] for par in (0, 1) for k in range(4)], first_lane, 16
            )
            for d, first in ((0, 0), (1, 72)):
                cor_out[fold, 2 * d + s] = packed(
                    [acc[par, q, first : first + 8] for par in (0, 1)], first_lane, 8
                )
        for copy in copies(fold):
            copy.start()

        for p in range(TILES):
            for par in (0, 1):
                m1, m2 = q1_v[par, p], q2_v[par, p]
                if par == 0:
                    above = jnp.concatenate([jnp.zeros((1, 128), F32), q1_v[1, p, : PAIRS - 1]], axis=0)
                else:
                    above = q1_v[0, p]
                    m1 = jnp.where((sub64 == PAIRS - 1) & bottom, 0.0, m1)
                before = roll(m2, 1)
                outer = roll(q2_v[par, p - 1], 1) if p else 0.0
                before = jnp.where(lane64 == 0, outer, before)
                if p + 1 == TILES:
                    m2 = jnp.where((lane64 == 127) & right, 0.0, m2)
                acc[par, p + 1, 8:72] = acc[par, p + 1, 8:72] - ((m1 - above) + (m2 - before))

        wait_in(fold)
        cols_add = [jnp.where(outside[2 + s], 0.0, col_in[fold, s]) for s in (0, 1)]
        cors_add = [jnp.where(outside[4 + s], 0.0, cor_in[fold, s]) for s in range(4)]
        for par in (0, 1):
            adds = []
            for s, first_lane in ((0, 0), (1, 112)):
                body = jnp.concatenate(
                    [unpacked(cols_add[s], 4 * par + k, first_lane) for k in range(4)], axis=0
                )
                zeros = jnp.zeros((PAIRS - 16, 128), F32)
                body = body + jnp.concatenate(
                    [unpacked(cors_add[s], par, first_lane), zeros, unpacked(cors_add[2 + s], par, first_lane)],
                    axis=0,
                )
                keep = lane64 < 15 if s == 0 else lane64 >= 113
                adds.append(jnp.where(keep, body, 0.0))
            for p in range(TILES):
                above = jnp.where(outside[0], 0.0, row_in[fold, 0, par, p])
                below = jnp.where(outside[1], 0.0, row_in[fold, 1, par, p])
                zeros = jnp.zeros((PAIRS - 16, 128), F32)
                value = acc[par, p + 1, 8:72] + jnp.concatenate([above, zeros, below], axis=0)
                if p == 0:
                    value = value + adds[0]
                if p + 1 == TILES:
                    value = value + adds[1]
                old = x_v[par, p]
                new = old - TAU * value
                x_v[par, p] = new
                bar_v[par, p] = 2.0 * new - old
        if step + 1 < ITERS:
            send_image(halo + 2)

    for par in (0, 1):
        for p in range(TILES):
            rows_of = pl.ds(par, PAIRS, stride=2)
            out_v[0, p, rows_of, :] = x_v[par, p]
            out_v[1, p, rows_of, :] = y_v[par, p]
    stores = [
        pltpu.make_async_copy(out_v.at[i, p], dst.at[:, slices[p]], store_sem.at[TILES * i + p])
        for i, dst in enumerate((restored_hbm, dual_out_hbm))
        for p in range(TILES)
    ]
    for store in stores:
        store.start()
    for store in stores:
        store.wait()


def per_device(observed, psf_table, psf_index, start_image, blur_dual, tv_dual):
    shape = observed.shape
    exchanges = 2 * ITERS
    block = (2, TILES, PAIRS, 128)
    tiled = (TILES, 2 * PAIRS, 128)
    hbm = pl.BlockSpec(memory_space=pl.ANY)
    return pl.pallas_call(
        kernel,
        out_shape=(jax.ShapeDtypeStruct(shape, F32), jax.ShapeDtypeStruct(shape, F32)),
        in_specs=[pl.BlockSpec(memory_space=pltpu.SMEM)] + [hbm] * 5,
        out_specs=(hbm, hbm),
        scratch_shapes=[
            pltpu.VMEM(tiled, F32),
            pltpu.VMEM(psf_table.shape, BF16),
            pltpu.VMEM(tiled, F32),
            pltpu.VMEM(tiled, F32),
            pltpu.VMEM((2,) + tiled, F32),
            pltpu.VMEM((2,) + tiled, F32),
            pltpu.VMEM((136, 128), F32),
            pltpu.VMEM((128, 128), F32),
            pltpu.VMEM((TILES * 4096, 128), BF16),
            pltpu.VMEM(block, F32),
            pltpu.VMEM(block, F32),
            pltpu.VMEM(block, F32),
            pltpu.VMEM(block, F32),
            pltpu.VMEM(block, F32),
            pltpu.VMEM(block, F32),
            pltpu.VMEM((2, 2, TILES, 88, 128), F32),
            pltpu.VMEM((2, TILES, 96, 128), F32),
            pltpu.VMEM((2, 2, TILES, 88, 128), F32),
            pltpu.VMEM((2, TILES + 2, 80, 128), F32),
            pltpu.VMEM((exchanges, 2, 2, TILES, 8, 128), F32),
            pltpu.VMEM((exchanges, 2, 16, 128), F32),
            pltpu.VMEM((exchanges, 4, 8, 128), F32),
            pltpu.VMEM((exchanges, 2, 2, TILES, 8, 128), F32),
            pltpu.VMEM((exchanges, 2, 16, 128), F32),
            pltpu.VMEM((exchanges, 4, 8, 128), F32),
            pltpu.SemaphoreType.DMA((4 * TILES + 1,)),
            pltpu.SemaphoreType.DMA((2 * TILES,)),
            pltpu.SemaphoreType.DMA((exchanges, 8)),
            pltpu.SemaphoreType.DMA((exchanges, 8)),
        ],
        compiler_params=pltpu.CompilerParams(collective_id=0, has_side_effects=True),
    )(psf_index, observed, psf_table, start_image, blur_dual, tv_dual)


def solution(mesh):
    placed = (
        P("row", "col"),
        P(),
        P("row", "col"),
        P("row", "col"),
        P("row", "col"),
        P(None, "row", "col"),
    )
    return jax.shard_map(
        per_device,
        mesh=mesh,
        in_specs=placed,
        out_specs=(P("row", "col"), P("row", "col")),
        check_vma=False,
    )
```

```python
import jax
import jax.numpy as jnp
from jax import lax
from jax.experimental import pallas as pl
from jax.experimental.pallas import tpu as pltpu
from jax.sharding import PartitionSpec as P

ITERS = 2
SIGMA = 0.15
TAU = 0.6
WEIGHT = 0.5
TAPS = 31
PAIRS = 64
TILES = 4
DIRS = ((-1, 0), (1, 0), (0, -1), (0, 1), (-1, -1), (-1, 1), (1, -1), (1, 1))
OPPOSITE = (1, 0, 3, 2, 7, 6, 5, 4)
MESH_ID = pl.DeviceIdType.MESH
F32 = jnp.float32
BF16 = jnp.bfloat16


def lanes(shape):
    return lax.broadcasted_iota(jnp.int32, shape, 1)


def roll(value, shift):
    shift = shift % 128
    return value if shift == 0 else pltpu.roll(value, shift, 1)


def kernel(
    index_ref, observed_hbm, table_hbm, start_hbm, dual_hbm, tv_hbm,
    restored_ref, dual_out_ref,
    start_v, table_v, observed_v, dual_v, tv_v,
    base_v, weights, x_v, bar_v, obs_v, y_v, q1_v, q2_v, shifted, ypad, spread, acc,
    row_out, col_out, cor_out, row_in, col_in, cor_in,
    load_sem, send_sem, recv_sem,
):
    row, col = lax.axis_index("row"), lax.axis_index("col")
    rows, cols = lax.axis_size("row"), lax.axis_size("col")

    def at(direction):
        dr, dc = direction
        return (lax.rem(row + dr + rows, rows), lax.rem(col + dc + cols, cols))

    top, bottom = row == 0, row == rows - 1
    left, right = col == 0, col == cols - 1
    outside = (top, bottom, left, right, top | left, top | right, bottom | left, bottom | right)
    inside = [jnp.logical_not(o) for o in outside]

    barrier = pltpu.get_barrier_semaphore()
    for d, direction in enumerate(DIRS):
        @pl.when(inside[d])
        def _():
            pl.semaphore_signal(barrier, inc=1, device_id=at(direction), device_id_type=MESH_ID)

    slices = [slice(128 * p, 128 * p + 128) for p in range(TILES)]
    plain = ((start_hbm, start_v), (observed_hbm, observed_v), (dual_hbm, dual_v))
    sources = [(src.at[:, slices[p]], dst.at[p]) for src, dst in plain for p in range(TILES)]
    sources += [(tv_hbm.at[:, :, slices[p]], tv_v.at[:, p]) for p in range(TILES)]
    sources.insert(TILES, (table_hbm, table_v))
    loads = [pltpu.make_async_copy(src, dst, load_sem.at[i]) for i, (src, dst) in enumerate(sources)]
    for load in loads:
        load.start()

    lane64 = lanes((PAIRS, 128))
    lane8 = lanes((8, 128))
    lane16 = lanes((16, 128))
    sub64 = lax.broadcasted_iota(jnp.int32, (PAIRS, 128), 0)

    def copies(exchange):
        result = []
        for d, direction in enumerate(DIRS):
            if d < 2:
                src, dst = row_out.at[exchange, d], row_in.at[exchange, d ^ 1]
            elif d < 4:
                src, dst = col_out.at[exchange, d - 2], col_in.at[exchange, (d - 2) ^ 1]
            else:
                src, dst = cor_out.at[exchange, d - 4], cor_in.at[exchange, 3 - (d - 4)]
            back = OPPOSITE[d]
            result.append(
                pltpu.make_async_remote_copy(
                    src_ref=src,
                    dst_ref=dst,
                    send_sem=send_sem.at[exchange, d],
                    recv_sem=recv_sem.at[exchange, back],
                    device_id=at(direction),
                    device_id_type=MESH_ID,
                )
            )
        return result

    def start_out(exchange):
        for d, copy in enumerate(copies(exchange)):
            pl.when(inside[d])(copy.start)

    def wait_in(exchange):
        for d, copy in enumerate(copies(exchange)):
            pl.when(inside[OPPOSITE[d]])(copy.wait_recv)

    def wait_out(exchange):
        for d, copy in enumerate(copies(exchange)):
            pl.when(inside[d])(copy.wait_send)

    def packed(parts, first_lane, height):
        lane = lane16 if height == 16 else lane8
        message = None
        for f, part in enumerate(parts):
            moved = roll(part, 16 * f - first_lane)
            message = moved if f == 0 else jnp.where(lane >= 16 * f, moved, message)
        return message

    def unpacked(message, f, first_lane):
        return roll(message, first_lane - 16 * f)

    for load in loads[:TILES]:
        load.wait()
    for par in (0, 1):
        for p in range(TILES):
            value = start_v[p, pl.ds(par, PAIRS, stride=2), :]
            x_v[par, p] = value
            bar_v[par, p] = value

    def send_image(exchange):
        for d, first in ((0, 0), (1, PAIRS - 8)):
            for par in (0, 1):
                for p in range(TILES):
                    row_out[exchange, d, par, p] = bar_v[par, p, first : first + 8]
        for s, (p, first_lane) in enumerate(((0, 0), (TILES - 1, 112))):
            col_out[exchange, s] = packed(
                [bar_v[par, p, 16 * k : 16 * k + 16] for par in (0, 1) for k in range(4)], first_lane, 16
            )
            for d, first in ((0, 0), (1, PAIRS - 8)):
                cor_out[exchange, 2 * d + s] = packed(
                    [bar_v[par, p, first : first + 8] for par in (0, 1)], first_lane, 8
                )
        start_out(exchange)

    pl.semaphore_wait(barrier, sum(i.astype(jnp.int32) for i in inside))
    send_image(0)

    loads[TILES].wait()
    which = lax.broadcasted_iota(jnp.int32, (8, 64), 0) & 3
    entry = lanes((8, 64))
    chosen = jnp.zeros((8, 64), F32)
    for p in range(TILES):
        chosen = jnp.where((which == p) & (entry == index_ref[0, p]), 1.0, chosen)
    chosen = chosen.astype(BF16)
    gap = jnp.zeros((1, 64), F32)
    lines = [
        jnp.concatenate([table_v[a].astype(F32), gap], axis=0).astype(BF16)
        if a < TAPS else jnp.zeros((32, 64), BF16)
        for a in range(32)
    ]
    picked = jnp.concatenate(
        [
            lax.dot_general(
                chosen,
                jnp.concatenate(lines[8 * k : 8 * k + 8], axis=0),
                (((1,), (1,)), ((), ())),
                preferred_element_type=F32,
            )
            for k in range(4)
        ],
        axis=1,
    )
    normed = picked / jnp.sum(picked, axis=1, keepdims=True)
    kernels = jnp.concatenate([normed[:, 128 * q : 128 * q + 128] for q in range(8)], axis=0)
    before = jnp.concatenate([jnp.zeros((8, 128), F32), kernels[:56]], axis=0)
    kernels, before = kernels.astype(BF16), before.astype(BF16)
    tap = lax.broadcasted_iota(jnp.int32, (128, 128), 0)
    place = lanes((128, 128))

    def flip(r, first):
        hit = ((tap >> 5) == r) & (place == ((first - (tap & 31)) & 127))
        return hit.astype(F32).astype(BF16)

    for r in range(4):
        low = jnp.dot(kernels, flip(r, 128), preferred_element_type=F32)
        high = jnp.dot(kernels if r else before, flip((r - 1) & 3, 64), preferred_element_type=F32)
        base_v[r] = low + high
    reach = tap - (place & 63)
    band = (reach >= 0) & (reach < TAPS)

    def build(step, carry):
        q, p = step >> 2, step & 3
        for r in range(4):
            line = jnp.broadcast_to(base_v[r, pl.ds(q * 8 + p, 1), :], (128, 128))
            rolled = pltpu.roll(line, 0, 1, stride=1, stride_axis=0)
            start = pl.multiple_of(p * 4096 + (q * 4 + r) * 128, 128)
            weights[pl.ds(start, 128), :] = jnp.where(band, rolled, 0.0).astype(BF16)
        return carry

    lax.fori_loop(0, 32, build, 0)

    ypad[...] = jnp.zeros_like(ypad)
    for load in loads[TILES + 1 :]:
        load.wait()
    for par in (0, 1):
        for p in range(TILES):
            rows_of = pl.ds(par, PAIRS, stride=2)
            obs_v[par, p] = observed_v[p, rows_of, :]
            y_v[par, p] = dual_v[p, rows_of, :]
            q1_v[par, p] = tv_v[0, p, rows_of, :]
            q2_v[par, p] = tv_v[1, p, rows_of, :]

    for step in range(ITERS):
        halo, fold = 2 * step, 2 * step + 1
        wait_in(halo)
        rows_in = [
            [
                [jnp.where(outside[d], 0.0, row_in[halo, d, par, p]) for p in range(TILES)]
                for par in (0, 1)
            ]
            for d in (0, 1)
        ]
        cols_in = [jnp.where(outside[2 + s], 0.0, col_in[halo, s]) for s in (0, 1)]
        cors_in = [jnp.where(outside[4 + s], 0.0, cor_in[halo, s]) for s in range(4)]

        def sides(par, first_lanes):
            return [
                jnp.concatenate(
                    [unpacked(cols_in[s], 4 * par + k, first_lanes[s]) for k in range(4)], axis=0
                )
                for s in (0, 1)
            ]

        def lay(tiles, par, first, count):
            lane = lanes((count, 128))
            by15 = [roll(t, 15) for t in tiles[:-1]]
            by79 = [roll(t, 79) for t in tiles[1:]]
            for p in range(TILES):
                shifted[par, 0, p, first : first + count] = jnp.where(lane < 15, by15[p], by15[p + 1])
                shifted[par, 1, p, first : first + count] = jnp.where(lane < 79, by79[p], by79[p + 1])

        side_tiles = [sides(par, (112, 0)) for par in (0, 1)]
        for par in (0, 1):
            lay(
                [side_tiles[par][0]] + [bar_v[par, p] for p in range(TILES)] + [side_tiles[par][1]], par, 8, PAIRS
            )
            for d, first in ((0, 0), (1, 72)):
                lay(
                    [unpacked(cors_in[2 * d], par, 112)]
                    + rows_in[d][par]
                    + [unpacked(cors_in[2 * d + 1], par, 0)],
                    par,
                    first,
                    8,
                )

        def blur(p, carry):
            pieces = []
            for t in range(16):
                pieces.append(
                    jnp.concatenate([shifted[0 + 1, h, p, t : t + PAIRS] for h in (0, 1)], axis=0).astype(BF16)
                )
                pieces.append(
                    jnp.concatenate([shifted[0, h, p, t + 1 : t + 1 + PAIRS] for h in (0, 1)], axis=0).astype(BF16)
                )
            stacked = jnp.concatenate(pieces, axis=1)
            matrix = weights[pl.ds(pl.multiple_of(p * 4096, 4096), 4096), :]
            blurred = jnp.dot(stacked, matrix, preferred_element_type=F32)
            first, second = blurred[:PAIRS], blurred[PAIRS:]
            even = jnp.where(lane64 < 64, first, roll(second, 64))
            odd = jnp.where(lane64 < 64, roll(first, 64), second)
            new = []
            for par, value in ((0, even), (1, odd)):
                updated = (y_v[par, p] + SIGMA * (value - obs_v[par, p])) / (1.0 + SIGMA)
                y_v[par, p] = updated
                new.append(updated)
            ypad[0, p, 16 : 16 + PAIRS] = jnp.where(lane64 < 64, new[0], roll(new[1], 64))
            ypad[1, p, 16 : 16 + PAIRS] = jnp.where(lane64 < 64, roll(new[0], 64), new[1])
            return carry

        lax.fori_loop(0, TILES, blur, 0)

        for p in range(TILES):
            even, odd = bar_v[0, p], bar_v[1, p]
            below = jnp.concatenate([even[1:], rows_in[1][0][p][:1]], axis=0)
            grad_even = odd - even
            grad_odd = jnp.where((sub64 == PAIRS - 1) & bottom, 0.0, below - odd)
            for par, value, grad1 in ((0, even, grad_even), (1, odd, grad_odd)):
                beyond = bar_v[par, p + 1] if p + 1 < TILES else side_tiles[par][1]
                after = jnp.where(lane64 < 127, roll(value, 127), roll(beyond, 127))
                grad2 = after - value
                if p + 1 == TILES:
                    grad2 = jnp.where((lane64 == 127) & right, 0.0, grad2)
                u1 = q1_v[par, p] + SIGMA * grad1
                u2 = q2_v[par, p] + SIGMA * grad2
                shrink = jnp.maximum(1.0, jnp.sqrt(u1 * u1 + u2 * u2) / WEIGHT)
                q1_v[par, p] = u1 / shrink
                q2_v[par, p] = u2 / shrink

        def adjoint(p, carry):
            pieces = [
                jnp.concatenate([ypad[h, p, 16 - t : 96 - t] for h in (0, 1)], axis=0).astype(BF16)
                for t in range(16)
            ]
            stacked = jnp.concatenate(pieces, axis=1)
            start = pl.multiple_of(p * 4096, 4096)
            matrix = jnp.concatenate(
                [weights[pl.ds(start + 256 * t, 256), :] for t in range(16)], axis=1
            )
            out = lax.dot_general(stacked, matrix, (((1,), (1,)), ((), ())), preferred_element_type=F32)
            for h in (0, 1):
                spread[1, h, p, 0:80] = out[80 * h : 80 * h + 80, 0:128]
                spread[0, h, p, 1:81] = out[80 * h : 80 * h + 80, 128:256]
            return carry

        lax.fori_loop(0, TILES, adjoint, 0)
        lane80 = lanes((80, 128))
        sub80 = lax.broadcasted_iota(jnp.int32, (80, 128), 0)
        for par in (0, 1):
            halves = [roll(spread[par, 1, p, 0:80], 64) for p in range(TILES)]
            total = []
            for q in range(TILES + 1):
                if q == 0:
                    value = spread[par, 0, 0, 0:80] + jnp.where(lane80 >= 64, halves[0], 0.0)
                elif q == TILES:
                    value = jnp.where(lane80 < 64, halves[q - 1], 0.0)
                else:
                    value = spread[par, 0, q, 0:80] + jnp.where(lane80 >= 64, halves[q], halves[q - 1])
                if par == 0:
                    value = jnp.where(sub80 == 0, 0.0, value)
                total.append(roll(value, 113))
            acc[par, 0] = jnp.where(lane80 >= 113, total[0], 0.0)
            for p in range(TILES):
                acc[par, p + 1] = jnp.where(lane80 < 113, total[p], total[p + 1])
            last = jnp.where(lane80 < 15, total[TILES], 0.0)
            acc[par, TILES + 1] = last
            acc[par, TILES + 1, 8:72] = last[8:72] + jnp.where(lane64 == 0, roll(q2_v[par, TILES - 1], 1), 0.0)

        for p in range(TILES):
            edge = jnp.concatenate([q1_v[1, p, PAIRS - 1 : PAIRS], jnp.zeros((7, 128), F32)], axis=0)
            acc[0, p + 1, 72:80] = acc[0, p + 1, 72:80] + edge
        for d, first in ((0, 0), (1, 72)):
            for par in (0, 1):
                for p in range(TILES):
                    row_out[fold, d, par, p] = acc[par, p + 1, first : first + 8]
        for s, (q, first_lane) in enumerate(((0, 112), (TILES + 1, 0))):
            col_out[fold, s] = packed(
                [acc[par, q, 8 + 16 * k : 24 + 16 * k] for par in (0, 1) for k in range(4)], first_lane, 16
            )
            for d, first in ((0, 0), (1, 72)):
                cor_out[fold, 2 * d + s] = packed(
                    [acc[par, q, first : first + 8] for par in (0, 1)], first_lane, 8
                )
        start_out(fold)

        for p in range(TILES):
            for par in (0, 1):
                m1, m2 = q1_v[par, p], q2_v[par, p]
                if par == 0:
                    above = jnp.concatenate([jnp.zeros((1, 128), F32), q1_v[1, p, : PAIRS - 1]], axis=0)
                else:
                    above = q1_v[0, p]
                    m1 = jnp.where((sub64 == PAIRS - 1) & bottom, 0.0, m1)
                before = roll(m2, 1)
                outer = roll(q2_v[par, p - 1], 1) if p else 0.0
                before = jnp.where(lane64 == 0, outer, before)
                if p + 1 == TILES:
                    m2 = jnp.where((lane64 == 127) & right, 0.0, m2)
                acc[par, p + 1, 8:72] = acc[par, p + 1, 8:72] - ((m1 - above) + (m2 - before))

        wait_in(fold)
        cols_add = [jnp.where(outside[2 + s], 0.0, col_in[fold, s]) for s in (0, 1)]
        cors_add = [jnp.where(outside[4 + s], 0.0, cor_in[fold, s]) for s in range(4)]
        for par in (0, 1):
            adds = []
            for s, first_lane in ((0, 0), (1, 112)):
                body = jnp.concatenate(
                    [unpacked(cols_add[s], 4 * par + k, first_lane) for k in range(4)], axis=0
                )
                zeros = jnp.zeros((PAIRS - 16, 128), F32)
                body = body + jnp.concatenate(
                    [unpacked(cors_add[s], par, first_lane), zeros, unpacked(cors_add[2 + s], par, first_lane)],
                    axis=0,
                )
                keep = lane64 < 15 if s == 0 else lane64 >= 113
                adds.append(jnp.where(keep, body, 0.0))
            for p in range(TILES):
                above = jnp.where(outside[0], 0.0, row_in[fold, 0, par, p])
                below = jnp.where(outside[1], 0.0, row_in[fold, 1, par, p])
                zeros = jnp.zeros((PAIRS - 16, 128), F32)
                value = acc[par, p + 1, 8:72] + jnp.concatenate([above, zeros, below], axis=0)
                if p == 0:
                    value = value + adds[0]
                if p + 1 == TILES:
                    value = value + adds[1]
                old = x_v[par, p]
                new = old - TAU * value
                x_v[par, p] = new
                bar_v[par, p] = 2.0 * new - old
        if step + 1 < ITERS:
            send_image(halo + 2)

    for par in (0, 1):
        for p in range(TILES):
            rows_of = pl.ds(par, PAIRS, stride=2)
            restored_ref[p, rows_of, :] = x_v[par, p]
            dual_out_ref[p, rows_of, :] = y_v[par, p]
    for exchange in range(2 * ITERS):
        wait_out(exchange)


def put_out(restored_ref, dual_ref, restored_hbm, dual_hbm, store_sem):
    stores = [
        pltpu.make_async_copy(src.at[p], dst.at[:, 128 * p : 128 * p + 128], store_sem.at[TILES * i + p])
        for i, (src, dst) in enumerate(((restored_ref, restored_hbm), (dual_ref, dual_hbm)))
        for p in range(TILES)
    ]
    for store in stores:
        store.start()
    for store in stores:
        store.wait()


def per_device(observed, psf_table, psf_index, start_image, blur_dual, tv_dual):
    shape = observed.shape
    exchanges = 2 * ITERS
    block = (2, TILES, PAIRS, 128)
    tiled = (TILES, 2 * PAIRS, 128)
    hbm = pl.BlockSpec(memory_space=pl.ANY)
    table = psf_table.transpose(1, 2, 0)
    results = pl.pallas_call(
        kernel,
        out_shape=(pltpu.VMEM(tiled, F32), pltpu.VMEM(tiled, F32)),
        in_specs=[pl.BlockSpec(memory_space=pltpu.SMEM)] + [hbm] * 5,
        out_specs=(pl.BlockSpec(memory_space=pltpu.VMEM),) * 2,
        scratch_shapes=[
            pltpu.VMEM(tiled, F32),
            pltpu.VMEM(table.shape, BF16),
            pltpu.VMEM(tiled, F32),
            pltpu.VMEM(tiled, F32),
            pltpu.VMEM((2,) + tiled, F32),
            pltpu.VMEM((4, 64, 128), F32),
            pltpu.VMEM((TILES * 4096, 128), BF16),
            pltpu.VMEM(block, F32),
            pltpu.VMEM(block, F32),
            pltpu.VMEM(block, F32),
            pltpu.VMEM(block, F32),
            pltpu.VMEM(block, F32),
            pltpu.VMEM(block, F32),
            pltpu.VMEM((2, 2, TILES, 88, 128), F32),
            pltpu.VMEM((2, TILES, 96, 128), F32),
            pltpu.VMEM((2, 2, TILES, 88, 128), F32),
            pltpu.VMEM((2, TILES + 2, 80, 128), F32),
            pltpu.VMEM((exchanges, 2, 2, TILES, 8, 128), F32),
            pltpu.VMEM((exchanges, 2, 16, 128), F32),
            pltpu.VMEM((exchanges, 4, 8, 128), F32),
            pltpu.VMEM((exchanges, 2, 2, TILES, 8, 128), F32),
            pltpu.VMEM((exchanges, 2, 16, 128), F32),
            pltpu.VMEM((exchanges, 4, 8, 128), F32),
            pltpu.SemaphoreType.DMA((4 * TILES + 1,)),
            pltpu.SemaphoreType.DMA((exchanges, 8)),
            pltpu.SemaphoreType.DMA((exchanges, 8)),
        ],
        compiler_params=pltpu.CompilerParams(collective_id=0, has_side_effects=True),
    )(psf_index, observed, table, start_image, blur_dual, tv_dual)
    return pl.pallas_call(
        put_out,
        out_shape=(jax.ShapeDtypeStruct(shape, F32), jax.ShapeDtypeStruct(shape, F32)),
        in_specs=[hbm] * 2,
        out_specs=(hbm, hbm),
        scratch_shapes=[pltpu.SemaphoreType.DMA((2 * TILES,))],
    )(*(pltpu.with_memory_space_constraint(result, pltpu.VMEM) for result in results))


def solution(mesh):
    placed = (
        P("row", "col"),
        P(),
        P("row", "col"),
        P("row", "col"),
        P("row", "col"),
        P(None, "row", "col"),
    )
    return jax.shard_map(
        per_device,
        mesh=mesh,
        in_specs=placed,
        out_specs=(P("row", "col"), P("row", "col")),
        check_vma=False,
    )
```

```python
import jax
import jax.numpy as jnp
from jax import lax
from jax.experimental import pallas as pl
from jax.experimental.pallas import tpu as pltpu
from jax.sharding import PartitionSpec as P

ITERS = 2
SIGMA = 0.15
TAU = 0.6
WEIGHT = 0.5
TAPS = 31
PAIRS = 64
TILES = 4
DIRS = ((-1, 0), (1, 0), (0, -1), (0, 1), (-1, -1), (-1, 1), (1, -1), (1, 1))
OPPOSITE = (1, 0, 3, 2, 7, 6, 5, 4)
MESH_ID = pl.DeviceIdType.MESH
F32 = jnp.float32
BF16 = jnp.bfloat16


def lanes(shape):
    return lax.broadcasted_iota(jnp.int32, shape, 1)


def roll(value, shift):
    shift = shift % 128
    return value if shift == 0 else pltpu.roll(value, shift, 1)


T_ROWS = 17 * 128


def kernel(
    index_ref, observed_hbm, table_hbm, start_hbm, dual_hbm, tv_hbm,
    restored_ref, dual_out_ref,
    start_v, table_v, observed_v, dual_v, tv_v,
    base_v, weights, weights_t, x_v, bar_v, obs_v, y_v, q1_v, q2_v, shifted, shifted_halo, blur_v, ypad, spread,
    row_out, col_out, cor_out, row_in, col_in, cor_in,
    load_sem, send_sem, recv_sem,
):
    row, col = lax.axis_index("row"), lax.axis_index("col")
    rows, cols = lax.axis_size("row"), lax.axis_size("col")

    def at(direction):
        dr, dc = direction
        return (lax.rem(row + dr + rows, rows), lax.rem(col + dc + cols, cols))

    top, bottom = row == 0, row == rows - 1
    left, right = col == 0, col == cols - 1
    outside = (top, bottom, left, right, top | left, top | right, bottom | left, bottom | right)
    inside = [jnp.logical_not(o) for o in outside]

    barrier = pltpu.get_barrier_semaphore()
    for d, direction in enumerate(DIRS):
        @pl.when(inside[d])
        def _():
            pl.semaphore_signal(barrier, inc=1, device_id=at(direction), device_id_type=MESH_ID)

    slices = [slice(128 * p, 128 * p + 128) for p in range(TILES)]
    plain = ((start_hbm, start_v), (observed_hbm, observed_v), (dual_hbm, dual_v))
    sources = [(src.at[:, slices[p]], dst.at[p]) for src, dst in plain for p in range(TILES)]
    sources += [(tv_hbm.at[:, :, slices[p]], tv_v.at[:, p]) for p in range(TILES)]
    sources.insert(TILES, (table_hbm, table_v))
    loads = [pltpu.make_async_copy(src, dst, load_sem.at[i]) for i, (src, dst) in enumerate(sources)]
    for load in loads:
        load.start()

    lane64 = lanes((PAIRS, 128))
    lane8 = lanes((8, 128))
    lane16 = lanes((16, 128))
    sub64 = lax.broadcasted_iota(jnp.int32, (PAIRS, 128), 0)

    def copies(exchange):
        result = []
        for d, direction in enumerate(DIRS):
            if d < 2:
                src, dst = row_out.at[exchange, d], row_in.at[exchange, d ^ 1]
            elif d < 4:
                src, dst = col_out.at[exchange, d - 2], col_in.at[exchange, (d - 2) ^ 1]
            else:
                src, dst = cor_out.at[exchange, d - 4], cor_in.at[exchange, 3 - (d - 4)]
            back = OPPOSITE[d]
            result.append(
                pltpu.make_async_remote_copy(
                    src_ref=src,
                    dst_ref=dst,
                    send_sem=send_sem.at[exchange, d],
                    recv_sem=recv_sem.at[exchange, back],
                    device_id=at(direction),
                    device_id_type=MESH_ID,
                )
            )
        return result

    def start_out(exchange):
        for d, copy in enumerate(copies(exchange)):
            pl.when(inside[d])(copy.start)

    def wait_in(exchange):
        for d, copy in enumerate(copies(exchange)):
            pl.when(inside[OPPOSITE[d]])(copy.wait_recv)

    def wait_out(exchange):
        for d, copy in enumerate(copies(exchange)):
            pl.when(inside[d])(copy.wait_send)

    def packed(parts, first_lane, height):
        lane = lane16 if height == 16 else lane8
        message = None
        for f, part in enumerate(parts):
            moved = roll(part, 16 * f - first_lane)
            message = moved if f == 0 else jnp.where(lane >= 16 * f, moved, message)
        return message

    def unpacked(message, f, first_lane):
        return roll(message, first_lane - 16 * f)

    for load in loads[:TILES]:
        load.wait()
    for par in (0, 1):
        for p in range(TILES):
            value = start_v[p, pl.ds(par, PAIRS, stride=2), :]
            x_v[par, p] = value
            bar_v[par, p] = value

    def send_image(exchange):
        for d, first in ((0, 0), (1, PAIRS - 8)):
            for par in (0, 1):
                for p in range(TILES):
                    row_out[exchange, d, par, p] = bar_v[par, p, first : first + 8]
        for s, (p, first_lane) in enumerate(((0, 0), (TILES - 1, 112))):
            col_out[exchange, s] = packed(
                [bar_v[par, p, 16 * k : 16 * k + 16] for par in (0, 1) for k in range(4)], first_lane, 16
            )
            for d, first in ((0, 0), (1, PAIRS - 8)):
                cor_out[exchange, 2 * d + s] = packed(
                    [bar_v[par, p, first : first + 8] for par in (0, 1)], first_lane, 8
                )
        start_out(exchange)

    pl.semaphore_wait(barrier, sum(i.astype(jnp.int32) for i in inside))
    send_image(0)

    loads[TILES].wait()
    which = lax.broadcasted_iota(jnp.int32, (8, 64), 0) & 3
    entry = lanes((8, 64))
    chosen = jnp.zeros((8, 64), F32)
    for p in range(TILES):
        chosen = jnp.where((which == p) & (entry == index_ref[0, p]), 1.0, chosen)
    chosen = chosen.astype(BF16)
    gap = jnp.zeros((1, 64), F32)
    lines = [
        jnp.concatenate([table_v[a].astype(F32), gap], axis=0).astype(BF16)
        if a < TAPS else jnp.zeros((32, 64), BF16)
        for a in range(32)
    ]
    picked = jnp.concatenate(
        [
            lax.dot_general(
                chosen,
                jnp.concatenate(lines[8 * k : 8 * k + 8], axis=0),
                (((1,), (1,)), ((), ())),
                preferred_element_type=F32,
            )
            for k in range(4)
        ],
        axis=1,
    )
    normed = picked / jnp.sum(picked, axis=1, keepdims=True)
    kernels = jnp.concatenate([normed[:, 128 * q : 128 * q + 128] for q in range(8)], axis=0)
    before = jnp.concatenate([jnp.zeros((8, 128), F32), kernels[:56]], axis=0)
    kernels, before = kernels.astype(BF16), before.astype(BF16)
    tap = lax.broadcasted_iota(jnp.int32, (128, 128), 0)
    place = lanes((128, 128))

    def flip(r, first):
        hit = ((tap >> 5) == r) & (place == ((first - (tap & 31)) & 127))
        return hit.astype(F32).astype(BF16)

    lane_of = lanes((64, 128))
    for r in range(4):
        low = jnp.dot(kernels, flip(r, 128), preferred_element_type=F32)
        high = jnp.dot(kernels if r else before, flip((r - 1) & 3, 64), preferred_element_type=F32)
        base_v[r] = low + high
        base_v[4 + r] = jnp.where(lane_of < 32, roll(kernels.astype(F32), -32 * r), 0.0)
    reach = tap - (place & 63)
    band = (reach >= 0) & (reach < TAPS)
    for p in range(TILES):
        weights_t[p * T_ROWS + 64 : p * T_ROWS + 128, 0:128] = jnp.zeros((64, 128), BF16)

    def build(q, carry):
        for p in range(TILES):
            for r in range(4):
                line = base_v[r, pl.ds(q * 8 + p, 1), :]
                rolled = pltpu.roll(jnp.broadcast_to(line, (128, 128)), 0, 1, stride=1, stride_axis=0)
                start = pl.multiple_of(p * 4096 + (q * 4 + r) * 128, 128)
                weights[pl.ds(start, 128), :] = jnp.where(band, rolled, 0.0).astype(BF16)
                line = base_v[4 + r, pl.ds(q * 8 + p, 1), :]
                rolled = pltpu.roll(jnp.broadcast_to(line, (64, 128)), 0, 1, stride=1, stride_axis=0).astype(BF16)
                for d in (0, 1):
                    t, e = (r + d) >> 1, (r + d) & 1
                    start = pl.multiple_of(p * T_ROWS + (q * 2 + t) * 128 + d * 64, 64)
                    weights_t[pl.ds(start, 64), 128 * e : 128 * e + 128] = rolled
        return carry

    lax.fori_loop(0, 8, build, 0)

    ypad[...] = jnp.zeros_like(ypad)
    shifted[...] = jnp.zeros_like(shifted)
    shifted_halo[...] = jnp.zeros_like(shifted_halo)
    for h in (0, 1):
        for p in range(TILES):
            spread[0, h, p, 0:8] = jnp.zeros((8, 128), F32)
    for load in loads[TILES + 1 :]:
        load.wait()
    for par in (0, 1):
        for p in range(TILES):
            rows_of = pl.ds(par, PAIRS, stride=2)
            obs_v[par, p] = observed_v[p, rows_of, :]
            y_v[par, p] = dual_v[p, rows_of, :]
            q1_v[par, p] = tv_v[0, p, rows_of, :]
            q2_v[par, p] = tv_v[1, p, rows_of, :]

    def stacked_rows(source, p, ranges):
        pieces = []
        for t in range(16):
            for par in (1, 0):
                first = t + 1 - par
                pieces.append(
                    jnp.concatenate(
                        [source[par, h, p, a + first : a + first + n] for h, a, n in ranges], axis=0
                    ).astype(BF16)
                )
        return jnp.concatenate(pieces, axis=1)

    def lay(target, tiles, par, first, count):
        lane = lanes((count, 128))
        by15 = [0.0 if t is None else roll(t, 15) for t in tiles[:-1]]
        by79 = [0.0 if t is None else roll(t, 79) for t in tiles[1:]]
        for p in range(TILES):
            target[par, 0, p, first : first + count] = jnp.where(lane < 15, by15[p], by15[p + 1])
            target[par, 1, p, first : first + count] = jnp.where(lane < 79, by79[p], by79[p + 1])

    def blur_own(p, carry):
        lhs = stacked_rows(shifted, p, ((0, 0, PAIRS), (1, 0, PAIRS)))
        matrix = weights[pl.ds(pl.multiple_of(p * 4096, 4096), 4096), :]
        blur_v[p] = jnp.dot(lhs, matrix, preferred_element_type=F32)
        return carry

    def tv(par, p, a, b, below, beyond):
        value = bar_v[par, p, a:b]
        if par == 0:
            grad1 = bar_v[1, p, a:b] - value
        elif b < PAIRS:
            grad1 = bar_v[0, p, a + 1 : b + 1] - value
        else:
            grad1 = jnp.concatenate([bar_v[0, p, a + 1 : b], below], axis=0) - value
            grad1 = jnp.where((lax.broadcasted_iota(jnp.int32, (b - a, 128), 0) == b - a - 1) & bottom, 0.0, grad1)
        if p + 1 < TILES:
            beyond = bar_v[par, p + 1, a:b]
        lane = lanes((b - a, 128))
        grad2 = jnp.where(lane < 127, roll(value, 127), roll(beyond, 127)) - value
        if p + 1 == TILES:
            grad2 = jnp.where((lane == 127) & right, 0.0, grad2)
        u1 = q1_v[par, p, a:b] + SIGMA * grad1
        u2 = q2_v[par, p, a:b] + SIGMA * grad2
        shrink = jnp.maximum(1.0, jnp.sqrt(u1 * u1 + u2 * u2) / WEIGHT)
        q1_v[par, p, a:b] = u1 / shrink
        q2_v[par, p, a:b] = u2 / shrink

    def merged(par, q, a, b):
        lane = lanes((b - a, 128))
        if q == 0:
            value = spread[par, 0, 0, a:b] + jnp.where(lane >= 64, roll(spread[par, 1, 0, a:b], 64), 0.0)
        elif q == TILES:
            value = jnp.where(lane < 64, roll(spread[par, 1, q - 1, a:b], 64), 0.0)
        else:
            value = spread[par, 0, q, a:b] + jnp.where(
                lane >= 64, roll(spread[par, 1, q, a:b], 64), roll(spread[par, 1, q - 1, a:b], 64)
            )
        return roll(value, 113)

    for step in range(ITERS):
        halo, fold = 2 * step, 2 * step + 1

        for par in (0, 1):
            lay(shifted, [None] + [bar_v[par, p] for p in range(TILES)] + [None], par, 8, PAIRS)
        lax.fori_loop(0, TILES, blur_own, 0)
        for p in range(TILES - 1):
            tv(0, p, 0, PAIRS, None, None)
            tv(1, p, 0, PAIRS - 8, None, None)

        wait_in(halo)
        rows_in = [
            [
                [jnp.where(outside[d], 0.0, row_in[halo, d, par, p]) for p in range(TILES)]
                for par in (0, 1)
            ]
            for d in (0, 1)
        ]
        cols_in = [jnp.where(outside[2 + s], 0.0, col_in[halo, s]) for s in (0, 1)]
        cors_in = [jnp.where(outside[4 + s], 0.0, cor_in[halo, s]) for s in range(4)]
        beyond = []
        for par in (0, 1):
            for d, first in ((0, 0), (1, 72)):
                lay(
                    shifted_halo,
                    [unpacked(cors_in[2 * d], par, 112)]
                    + rows_in[d][par]
                    + [unpacked(cors_in[2 * d + 1], par, 0)],
                    par,
                    first,
                    8,
                )
            for k in range(4):
                side = [unpacked(cols_in[0], 4 * par + k, 112 + 15), unpacked(cols_in[1], 4 * par + k, 79)]
                place_k = slice(8 + 16 * k, 24 + 16 * k)
                shifted_halo[par, 0, 0, place_k] = jnp.where(lane16 < 15, side[0], 0.0)
                shifted_halo[par, 1, TILES - 1, place_k] = jnp.where(lane16 < 79, 0.0, side[1])
            beyond.append(jnp.concatenate([unpacked(cols_in[1], 4 * par + k, 0) for k in range(4)], axis=0))

        gap48 = jnp.zeros((PAIRS - 16, 128), F32)

        def rows_full(p):
            return 0 if p == 0 else 1 if p + 1 == TILES else None

        def blur_halo(p):
            full = rows_full(p)
            ranges = [(full, 0, PAIRS)] if full is not None else []
            for h in (0, 1):
                if h != full:
                    ranges += [(h, 0, 8), (h, PAIRS - 8, 8)]
            return jnp.dot(
                stacked_rows(shifted_halo, p, ranges),
                weights[p * 4096 : p * 4096 + 4096],
                preferred_element_type=F32,
            )

        def dual(p, extra):
            full = rows_full(p)
            halves, place_r = [None, None], 0
            if full is not None:
                halves[full] = blur_v[p, PAIRS * full : PAIRS * full + PAIRS] + extra[:PAIRS]
                place_r = PAIRS
            for h in (0, 1):
                if h != full:
                    more = jnp.concatenate(
                        [extra[place_r : place_r + 8], gap48, extra[place_r + 8 : place_r + 16]], axis=0
                    )
                    halves[h] = blur_v[p, PAIRS * h : PAIRS * h + PAIRS] + more
                    place_r += 16
            even = jnp.where(lane64 < 64, halves[0], roll(halves[1], 64))
            odd = jnp.where(lane64 < 64, roll(halves[0], 64), halves[1])
            new = []
            for par, value in ((0, even), (1, odd)):
                updated = (y_v[par, p] + SIGMA * (value - obs_v[par, p])) / (1.0 + SIGMA)
                y_v[par, p] = updated
                new.append(updated)
            ypad[0, p, 16 : 16 + PAIRS] = jnp.where(lane64 < 64, new[0], roll(new[1], 64))
            ypad[1, p, 16 : 16 + PAIRS] = jnp.where(lane64 < 64, roll(new[0], 64), new[1])

        def adjoint(p):
            out = jnp.dot(
                jnp.concatenate(
                    [
                        jnp.concatenate([ypad[h, p, 16 - t : 96 - t] for h in (0, 1)], axis=0).astype(BF16)
                        for t in range(16)
                    ],
                    axis=1,
                ),
                weights_t[p * T_ROWS : p * T_ROWS + 2048],
                preferred_element_type=F32,
            )
            for h in (0, 1):
                spread[1, h, p, 0:80] = out[80 * h : 80 * h + 80, 0:128]
                spread[0, h, p, 1:81] = out[80 * h : 80 * h + 80, 128:256]

        extras = [blur_halo(p) for p in range(TILES)]
        for p in range(TILES):
            dual(p, extras[p])
        for p in range(TILES):
            adjoint(p)

        for p in range(TILES - 1):
            tv(1, p, PAIRS - 8, PAIRS, rows_in[1][0][p][:1], None)
        for par in (0, 1):
            tv(par, TILES - 1, 0, PAIRS, rows_in[1][0][TILES - 1][:1], beyond[par])

        corners = [[None, None] for _ in range(4)]
        for par in (0, 1):
            for d, (a, b) in ((0, (0, 8)), (1, (72, 80))):
                tiles = [merged(par, q, a, b) for q in range(TILES + 1)]
                for p in range(TILES):
                    value = jnp.where(lane8 < 113, tiles[p], tiles[p + 1])
                    if d == 1 and par == 0:
                        value = value + jnp.concatenate(
                            [q1_v[1, p, PAIRS - 1 : PAIRS], jnp.zeros((7, 128), F32)], axis=0
                        )
                    row_out[fold, d, par, p] = value
                corners[2 * d][par] = jnp.where(lane8 >= 113, tiles[0], 0.0)
                corners[2 * d + 1][par] = jnp.where(lane8 < 15, tiles[TILES], 0.0)
        sides = [[None, None], [None, None]]
        for par in (0, 1):
            sides[0][par] = jnp.where(lane64 >= 113, merged(par, 0, 8, 72), 0.0)
            sides[1][par] = jnp.where(lane64 < 15, merged(par, TILES, 8, 72), 0.0) + jnp.where(
                lane64 == 0, roll(q2_v[par, TILES - 1], 1), 0.0
            )
        for s, first_lane in enumerate((112, 0)):
            col_out[fold, s] = packed(
                [sides[s][par][16 * k : 16 * k + 16] for par in (0, 1) for k in range(4)], first_lane, 16
            )
            for d in (0, 1):
                cor_out[fold, 2 * d + s] = packed(corners[2 * d + s], first_lane, 8)
        start_out(fold)

        for par in (0, 1):
            tiles = [merged(par, q, 8, 72) for q in range(TILES + 1)]
            for p in range(TILES):
                value = jnp.where(lane64 < 113, tiles[p], tiles[p + 1])
                m1, m2 = q1_v[par, p], q2_v[par, p]
                if par == 0:
                    above = jnp.concatenate([jnp.zeros((1, 128), F32), q1_v[1, p, : PAIRS - 1]], axis=0)
                else:
                    above = q1_v[0, p]
                    m1 = jnp.where((sub64 == PAIRS - 1) & bottom, 0.0, m1)
                outer = roll(q2_v[par, p - 1], 1) if p else 0.0
                before = jnp.where(lane64 == 0, outer, roll(m2, 1))
                if p + 1 == TILES:
                    m2 = jnp.where((lane64 == 127) & right, 0.0, m2)
                value = value - ((m1 - above) + (m2 - before))
                old = x_v[par, p]
                new = old - TAU * value
                x_v[par, p] = new
                bar_v[par, p] = 2.0 * new - old
        if step + 1 == ITERS:
            for par in (0, 1):
                for p in range(TILES):
                    dual_out_ref[p, pl.ds(par, PAIRS, stride=2), :] = y_v[par, p]

        wait_in(fold)

        def subtract(par, p, a, b, value):
            x_v[par, p, a:b] = x_v[par, p, a:b] - TAU * value
            bar_v[par, p, a:b] = bar_v[par, p, a:b] - 2.0 * TAU * value

        for par in (0, 1):
            for s, p, first_lane in ((0, 0, 0), (1, TILES - 1, 112)):
                message = jnp.where(outside[2 + s], 0.0, col_in[fold, s])
                keep = lane16 < 15 if s == 0 else lane16 >= 113
                for k in range(4):
                    value = jnp.where(keep, unpacked(message, 4 * par + k, first_lane), 0.0)
                    subtract(par, p, 16 * k, 16 * k + 16, value)
            for d, (a, b) in ((0, (0, 8)), (1, (PAIRS - 8, PAIRS))):
                for p in range(TILES):
                    value = jnp.where(outside[d], 0.0, row_in[fold, d, par, p])
                    if p in (0, TILES - 1):
                        s = 0 if p == 0 else 1
                        message = jnp.where(outside[4 + 2 * d + s], 0.0, cor_in[fold, 2 * d + s])
                        keep = lane8 < 15 if s == 0 else lane8 >= 113
                        value = value + jnp.where(keep, unpacked(message, par, 112 * s), 0.0)
                    subtract(par, p, a, b, value)
        if step + 1 < ITERS:
            send_image(halo + 2)

    for par in (0, 1):
        for p in range(TILES):
            restored_ref[p, pl.ds(par, PAIRS, stride=2), :] = x_v[par, p]
    for exchange in range(2 * ITERS):
        wait_out(exchange)


def put_out(restored_ref, dual_ref, restored_hbm, dual_hbm, store_sem):
    stores = [
        pltpu.make_async_copy(src.at[p], dst.at[:, 128 * p : 128 * p + 128], store_sem.at[TILES * i + p])
        for i, (src, dst) in enumerate(((restored_ref, restored_hbm), (dual_ref, dual_hbm)))
        for p in range(TILES)
    ]
    for store in stores:
        store.start()
    for store in stores:
        store.wait()


def per_device(observed, psf_table, psf_index, start_image, blur_dual, tv_dual):
    shape = observed.shape
    exchanges = 2 * ITERS
    block = (2, TILES, PAIRS, 128)
    tiled = (TILES, 2 * PAIRS, 128)
    hbm = pl.BlockSpec(memory_space=pl.ANY)
    table = psf_table.transpose(1, 2, 0)
    results = pl.pallas_call(
        kernel,
        out_shape=(pltpu.VMEM(tiled, F32), pltpu.VMEM(tiled, F32)),
        in_specs=[pl.BlockSpec(memory_space=pltpu.SMEM)] + [hbm] * 5,
        out_specs=(pl.BlockSpec(memory_space=pltpu.VMEM),) * 2,
        scratch_shapes=[
            pltpu.VMEM(tiled, F32),
            pltpu.VMEM(table.shape, BF16),
            pltpu.VMEM(tiled, F32),
            pltpu.VMEM(tiled, F32),
            pltpu.VMEM((2,) + tiled, F32),
            pltpu.VMEM((8, 64, 128), F32),
            pltpu.VMEM((TILES * 4096, 128), BF16),
            pltpu.VMEM((TILES * T_ROWS, 256), BF16),
            pltpu.VMEM(block, F32),
            pltpu.VMEM(block, F32),
            pltpu.VMEM(block, F32),
            pltpu.VMEM(block, F32),
            pltpu.VMEM(block, F32),
            pltpu.VMEM(block, F32),
            pltpu.VMEM((2, 2, TILES, 80, 128), F32),
            pltpu.VMEM((2, 2, TILES, 80, 128), F32),
            pltpu.VMEM((TILES, 128, 128), F32),
            pltpu.VMEM((2, TILES, 96, 128), F32),
            pltpu.VMEM((2, 2, TILES, 88, 128), F32),
            pltpu.VMEM((exchanges, 2, 2, TILES, 8, 128), F32),
            pltpu.VMEM((exchanges, 2, 16, 128), F32),
            pltpu.VMEM((exchanges, 4, 8, 128), F32),
            pltpu.VMEM((exchanges, 2, 2, TILES, 8, 128), F32),
            pltpu.VMEM((exchanges, 2, 16, 128), F32),
            pltpu.VMEM((exchanges, 4, 8, 128), F32),
            pltpu.SemaphoreType.DMA((4 * TILES + 1,)),
            pltpu.SemaphoreType.DMA((exchanges, 8)),
            pltpu.SemaphoreType.DMA((exchanges, 8)),
        ],
        compiler_params=pltpu.CompilerParams(collective_id=0, has_side_effects=True),
    )(psf_index, observed, table, start_image, blur_dual, tv_dual)
    return pl.pallas_call(
        put_out,
        out_shape=(jax.ShapeDtypeStruct(shape, F32), jax.ShapeDtypeStruct(shape, F32)),
        in_specs=[hbm] * 2,
        out_specs=(hbm, hbm),
        scratch_shapes=[pltpu.SemaphoreType.DMA((2 * TILES,))],
    )(*(pltpu.with_memory_space_constraint(result, pltpu.VMEM) for result in results))


def solution(mesh):
    placed = (
        P("row", "col"),
        P(),
        P("row", "col"),
        P("row", "col"),
        P("row", "col"),
        P(None, "row", "col"),
    )
    return jax.shard_map(
        per_device,
        mesh=mesh,
        in_specs=placed,
        out_specs=(P("row", "col"), P("row", "col")),
        check_vma=False,
    )
```

```python
import jax
import jax.numpy as jnp
from jax import lax
from jax.experimental import pallas as pl
from jax.experimental.pallas import tpu as pltpu
from jax.sharding import PartitionSpec as P

EXCHANGES = 3
SIGMA = 0.15
TAU = 0.6
WEIGHT = 0.5
TAPS = 31
PAIRS = 64
TILES = 4
DIRS = ((-1, 0), (1, 0), (0, -1), (0, 1), (-1, -1), (-1, 1), (1, -1), (1, 1))
OPPOSITE = (1, 0, 3, 2, 7, 6, 5, 4)
MESH_ID = pl.DeviceIdType.MESH
F32 = jnp.float32
BF16 = jnp.bfloat16


def lanes(shape):
    return lax.broadcasted_iota(jnp.int32, shape, 1)


def roll(value, shift):
    shift = shift % 128
    return value if shift == 0 else pltpu.roll(value, shift, 1)


T_ROWS = 17 * 128


def kernel(
    index_hbm, observed_hbm, table_hbm, start_hbm, dual_hbm, tv_hbm,
    restored_ref, dual_out_ref,
    start_v, table_v, index_ref, observed_v, dual_v, tv_v,
    base_v, weights, weights_t, x_e, bar_e, acc, obs_v, y_v, q1_v, q2_v, shifted, shifted_halo, blur_v, ypad, spread,
    row_out, col_out, cor_out, row_in, col_in, cor_in,
    wide_row_out, wide_col_out, wide_cor_out, wide_row_in, wide_col_in, wide_cor_in,
    load_sem, send_sem, recv_sem,
):
    row, col = lax.axis_index("row"), lax.axis_index("col")
    rows, cols = lax.axis_size("row"), lax.axis_size("col")

    def at(direction):
        dr, dc = direction
        return (lax.rem(row + dr + rows, rows), lax.rem(col + dc + cols, cols))

    top, bottom = row == 0, row == rows - 1
    left, right = col == 0, col == cols - 1
    outside = (top, bottom, left, right, top | left, top | right, bottom | left, bottom | right)
    inside = [jnp.logical_not(o) for o in outside]

    barrier = pltpu.get_barrier_semaphore()
    for d, direction in enumerate(DIRS):
        @pl.when(inside[d])
        def _():
            pl.semaphore_signal(barrier, inc=1, device_id=at(direction), device_id_type=MESH_ID)

    slices = [slice(128 * p, 128 * p + 128) for p in range(TILES)]
    plain = ((start_hbm, start_v), (observed_hbm, observed_v), (dual_hbm, dual_v))
    sources = [(src.at[:, slices[p]], dst.at[p]) for src, dst in plain for p in range(TILES)]
    sources += [(tv_hbm.at[:, :, slices[p]], tv_v.at[:, p]) for p in range(TILES)]
    sources[TILES:TILES] = [(table_hbm, table_v), (index_hbm, index_ref)]
    loads = [pltpu.make_async_copy(src, dst, load_sem.at[i]) for i, (src, dst) in enumerate(sources)]
    for load in loads:
        load.start()

    lane64 = lanes((PAIRS, 128))
    lane8 = lanes((8, 128))
    lane16 = lanes((16, 128))

    wide = (wide_row_out, wide_col_out, wide_cor_out, wide_row_in, wide_col_in, wide_cor_in)
    narrow = (row_out, col_out, cor_out, row_in, col_in, cor_in)

    def copies(exchange):
        refs = wide if exchange == 1 else [ref.at[exchange // 2] for ref in narrow]
        result = []
        for d, direction in enumerate(DIRS):
            if d < 2:
                src, dst = refs[0].at[d], refs[3].at[d ^ 1]
            elif d < 4:
                src, dst = refs[1].at[d - 2], refs[4].at[(d - 2) ^ 1]
            else:
                src, dst = refs[2].at[d - 4], refs[5].at[3 - (d - 4)]
            back = OPPOSITE[d]
            result.append(
                pltpu.make_async_remote_copy(
                    src_ref=src,
                    dst_ref=dst,
                    send_sem=send_sem.at[exchange, d],
                    recv_sem=recv_sem.at[exchange, back],
                    device_id=at(direction),
                    device_id_type=MESH_ID,
                )
            )
        return result

    def start_out(exchange):
        for d, copy in enumerate(copies(exchange)):
            pl.when(inside[d])(copy.start)

    def wait_in(exchange):
        for d, copy in enumerate(copies(exchange)):
            pl.when(inside[OPPOSITE[d]])(copy.wait_recv)

    def wait_out(exchange):
        for d, copy in enumerate(copies(exchange)):
            pl.when(inside[d])(copy.wait_send)

    def packed(parts, first_lane, height):
        lane = lane16 if height == 16 else lane8
        message = None
        for f, part in enumerate(parts):
            moved = roll(part, 16 * f - first_lane)
            message = moved if f == 0 else jnp.where(lane >= 16 * f, moved, message)
        return message

    def unpacked(message, f, first_lane):
        return roll(message, first_lane - 16 * f)

    x_e[...] = jnp.zeros_like(x_e)
    bar_e[...] = jnp.zeros_like(bar_e)
    for load in loads[:TILES]:
        load.wait()
    for par in (0, 1):
        for p in range(TILES):
            value = start_v[p, pl.ds(par, PAIRS, stride=2), :]
            x_e[par, p + 1, 8:72] = value
            bar_e[par, p + 1, 8:72] = value
    for d, first in ((0, 8), (1, 64)):
        for par in (0, 1):
            for p in range(TILES):
                row_out[0, d, par, p] = bar_e[par, p + 1, first : first + 8]
    for s, (q, first_lane) in enumerate(((1, 0), (TILES, 112))):
        col_out[0, s] = packed(
            [bar_e[par, q, 8 + 16 * k : 24 + 16 * k] for par in (0, 1) for k in range(4)], first_lane, 16
        )
        for d, first in ((0, 8), (1, 64)):
            cor_out[0, 2 * d + s] = packed([bar_e[par, q, first : first + 8] for par in (0, 1)], first_lane, 8)

    pl.semaphore_wait(barrier, sum(i.astype(jnp.int32) for i in inside))
    start_out(0)

    for load in loads[TILES : TILES + 2]:
        load.wait()
    which = lax.broadcasted_iota(jnp.int32, (8, 64), 0) & 3
    entry = lanes((8, 64))
    chosen = jnp.zeros((8, 64), F32)
    for p in range(TILES):
        chosen = jnp.where((which == p) & (entry == index_ref[0, p]), 1.0, chosen)
    chosen = chosen.astype(BF16)
    gap = jnp.zeros((1, 64), F32)
    lines = [
        jnp.concatenate([table_v[a].astype(F32), gap], axis=0).astype(BF16)
        if a < TAPS else jnp.zeros((32, 64), BF16)
        for a in range(32)
    ]
    picked = jnp.concatenate(
        [
            lax.dot_general(
                chosen,
                jnp.concatenate(lines[8 * k : 8 * k + 8], axis=0),
                (((1,), (1,)), ((), ())),
                preferred_element_type=F32,
            )
            for k in range(4)
        ],
        axis=1,
    )
    normed = picked / jnp.sum(picked, axis=1, keepdims=True)
    kernels = jnp.concatenate([normed[:, 128 * q : 128 * q + 128] for q in range(8)], axis=0)
    before = jnp.concatenate([jnp.zeros((8, 128), F32), kernels[:56]], axis=0)
    kernels, before = kernels.astype(BF16), before.astype(BF16)
    tap = lax.broadcasted_iota(jnp.int32, (128, 128), 0)
    place = lanes((128, 128))

    def flip(r, first):
        hit = ((tap >> 5) == r) & (place == ((first - (tap & 31)) & 127))
        return hit.astype(F32).astype(BF16)

    lane_of = lanes((64, 128))
    for r in range(4):
        low = jnp.dot(kernels, flip(r, 128), preferred_element_type=F32)
        high = jnp.dot(kernels if r else before, flip((r - 1) & 3, 64), preferred_element_type=F32)
        base_v[r] = low + high
        base_v[4 + r] = jnp.where(lane_of < 32, roll(kernels.astype(F32), -32 * r), 0.0)
    reach = tap - (place & 63)
    band = (reach >= 0) & (reach < TAPS)
    for p in range(TILES):
        weights_t[p * T_ROWS + 64 : p * T_ROWS + 128, 0:128] = jnp.zeros((64, 128), BF16)

    def build(q, carry):
        for p in range(TILES):
            for r in range(4):
                line = base_v[r, pl.ds(q * 8 + p, 1), :]
                rolled = pltpu.roll(jnp.broadcast_to(line, (128, 128)), 0, 1, stride=1, stride_axis=0)
                start = pl.multiple_of(p * 4096 + (q * 4 + r) * 128, 128)
                weights[pl.ds(start, 128), :] = jnp.where(band, rolled, 0.0).astype(BF16)
                line = base_v[4 + r, pl.ds(q * 8 + p, 1), :]
                rolled = pltpu.roll(jnp.broadcast_to(line, (64, 128)), 0, 1, stride=1, stride_axis=0).astype(BF16)
                for d in (0, 1):
                    t, e = (r + d) >> 1, (r + d) & 1
                    start = pl.multiple_of(p * T_ROWS + (q * 2 + t) * 128 + d * 64, 64)
                    weights_t[pl.ds(start, 64), 128 * e : 128 * e + 128] = rolled
        return carry

    lax.fori_loop(0, 8, build, 0)

    ypad[...] = jnp.zeros_like(ypad)
    shifted[...] = jnp.zeros_like(shifted)
    shifted_halo[...] = jnp.zeros_like(shifted_halo)
    for h in (0, 1):
        for p in range(TILES):
            spread[0, h, p, 0:8] = jnp.zeros((8, 128), F32)
    for load in loads[TILES + 2 :]:
        load.wait()
    for par in (0, 1):
        for p in range(TILES):
            rows_of = pl.ds(par, PAIRS, stride=2)
            obs_v[par, p] = observed_v[p, rows_of, :]
            y_v[par, p] = dual_v[p, rows_of, :]
            q1_v[par, p] = tv_v[0, p, rows_of, :]
            q2_v[par, p] = tv_v[1, p, rows_of, :]

    def stacked_rows(source, p, ranges):
        pieces = []
        for t in range(16):
            for par in (1, 0):
                first = t + 1 - par
                pieces.append(
                    jnp.concatenate(
                        [source[par, h, p, a + first : a + first + n] for h, a, n in ranges], axis=0
                    ).astype(BF16)
                )
        return jnp.concatenate(pieces, axis=1)

    def lay(target, par, a, b):
        lane = lanes((b - a, 128))
        tiles = [bar_e[par, q, a:b] for q in range(TILES + 2)]
        by15 = [roll(t, 15) for t in tiles[:-1]]
        by79 = [roll(t, 79) for t in tiles[1:]]
        for p in range(TILES):
            target[par, 0, p, a:b] = jnp.where(lane < 15, by15[p], by15[p + 1])
            target[par, 1, p, a:b] = jnp.where(lane < 79, by79[p], by79[p + 1])

    def lay_sides(par, a, b, reach_in):
        lane = lanes((b - a, 128))
        first = jnp.where(lane < 15, roll(bar_e[par, 0, a:b], 15), roll(bar_e[par, 1, a:b], 15))
        last = jnp.where(lane < 79, roll(bar_e[par, TILES, a:b], 79), roll(bar_e[par, TILES + 1, a:b], 79))
        shifted_halo[par, 0, 0, a:b] = jnp.where(lane < 15 + reach_in, first, 0.0)
        shifted_halo[par, 1, TILES - 1, a:b] = jnp.where(lane >= 79 - reach_in, last, 0.0)

    def blur_own(p, carry):
        lhs = stacked_rows(shifted, p, ((0, 0, PAIRS), (1, 0, PAIRS)))
        matrix = weights[pl.ds(pl.multiple_of(p * 4096, 4096), 4096), :]
        blur_v[p] = jnp.dot(lhs, matrix, preferred_element_type=F32)
        return carry

    def tv(par, p, a, b):
        value = bar_e[par, p + 1, a + 8 : b + 8]
        if par == 0:
            grad1 = bar_e[1, p + 1, a + 8 : b + 8] - value
        else:
            grad1 = bar_e[0, p + 1, a + 9 : b + 9] - value
            if b == PAIRS:
                grad1 = jnp.where(
                    (lax.broadcasted_iota(jnp.int32, (b - a, 128), 0) == b - a - 1) & bottom, 0.0, grad1
                )
        lane = lanes((b - a, 128))
        grad2 = jnp.where(lane < 127, roll(value, 127), roll(bar_e[par, p + 2, a + 8 : b + 8], 127)) - value
        if p + 1 == TILES:
            grad2 = jnp.where((lane == 127) & right, 0.0, grad2)
        u1 = q1_v[par, p, a:b] + SIGMA * grad1
        u2 = q2_v[par, p, a:b] + SIGMA * grad2
        shrink = jnp.maximum(1.0, jnp.sqrt(u1 * u1 + u2 * u2) / WEIGHT)
        q1_v[par, p, a:b] = u1 / shrink
        q2_v[par, p, a:b] = u2 / shrink

    def merged(par, q, a, b):
        lane = lanes((b - a, 128))
        if q == 0:
            value = spread[par, 0, 0, a:b] + jnp.where(lane >= 64, roll(spread[par, 1, 0, a:b], 64), 0.0)
        elif q == TILES:
            value = jnp.where(lane < 64, roll(spread[par, 1, q - 1, a:b], 64), 0.0)
        else:
            value = spread[par, 0, q, a:b] + jnp.where(
                lane >= 64, roll(spread[par, 1, q, a:b], 64), roll(spread[par, 1, q - 1, a:b], 64)
            )
        return roll(value, 113)

    def own_part(par, p, a, b, tiles):
        lane = lanes((b - a, 128))
        sub = lax.broadcasted_iota(jnp.int32, (b - a, 128), 0)
        i, j = a - 8, b - 8
        m1, m2 = q1_v[par, p, i:j], q2_v[par, p, i:j]
        if par == 1:
            above = q1_v[0, p, i:j]
            if b == 72:
                m1 = jnp.where((sub == b - a - 1) & bottom, 0.0, m1)
        elif a == 8:
            above = jnp.concatenate([jnp.zeros((1, 128), F32), q1_v[1, p, : j - 1]], axis=0)
        else:
            above = q1_v[1, p, i - 1 : j - 1]
        outer = roll(q2_v[par, p - 1, i:j], 1) if p else 0.0
        before = jnp.where(lane == 0, outer, roll(m2, 1))
        if p + 1 == TILES:
            m2 = jnp.where((lane == 127) & right, 0.0, m2)
        return jnp.where(lane < 113, tiles[p], tiles[p + 1]) - ((m1 - above) + (m2 - before))

    def rim_part(par, p, d, tiles):
        value = jnp.where(lane8 < 113, tiles[p], tiles[p + 1])
        if d == 1 and par == 0:
            edge = jnp.concatenate([q1_v[1, p, PAIRS - 1 : PAIRS], jnp.zeros((7, 128), F32)], axis=0)
            value = value + edge
        return value

    def side_part(par, s, a, b, tile):
        lane = lanes((b - a, 128))
        if s == 0:
            return jnp.where(lane >= 113, tile, 0.0)
        value = jnp.where(lane < 15, tile, 0.0)
        if 8 <= a < 72:
            value = value + jnp.where(lane == 0, roll(q2_v[par, TILES - 1, a - 8 : b - 8], 1), 0.0)
        return value

    def masked(direction, value):
        return jnp.where(outside[direction], 0.0, value)

    def duals(edge):
        gap = jnp.zeros((PAIRS - 2 * edge, 128), F32)

        def rows_full(p):
            return 0 if p == 0 else 1 if p + 1 == TILES else None

        def blur_halo(p):
            full = rows_full(p)
            ranges = [(full, 0, PAIRS)] if full is not None else []
            for h in (0, 1):
                if h != full:
                    ranges += [(h, 0, edge), (h, PAIRS - edge, edge)]
            return jnp.dot(
                stacked_rows(shifted_halo, p, ranges),
                weights[p * 4096 : p * 4096 + 4096],
                preferred_element_type=F32,
            )

        def dual(p, extra):
            full = rows_full(p)
            halves, place_r = [None, None], 0
            if full is not None:
                halves[full] = blur_v[p, PAIRS * full : PAIRS * full + PAIRS] + extra[:PAIRS]
                place_r = PAIRS
            for h in (0, 1):
                if h != full:
                    more = jnp.concatenate(
                        [extra[place_r : place_r + edge], gap, extra[place_r + edge : place_r + 2 * edge]], axis=0
                    )
                    halves[h] = blur_v[p, PAIRS * h : PAIRS * h + PAIRS] + more
                    place_r += 2 * edge
            even = jnp.where(lane64 < 64, halves[0], roll(halves[1], 64))
            odd = jnp.where(lane64 < 64, roll(halves[0], 64), halves[1])
            new = []
            for par, value in ((0, even), (1, odd)):
                updated = (y_v[par, p] + SIGMA * (value - obs_v[par, p])) / (1.0 + SIGMA)
                y_v[par, p] = updated
                new.append(updated)
            ypad[0, p, 16 : 16 + PAIRS] = jnp.where(lane64 < 64, new[0], roll(new[1], 64))
            ypad[1, p, 16 : 16 + PAIRS] = jnp.where(lane64 < 64, roll(new[0], 64), new[1])

        def adjoint(p):
            out = jnp.dot(
                jnp.concatenate(
                    [
                        jnp.concatenate([ypad[h, p, 16 - t : 96 - t] for h in (0, 1)], axis=0).astype(BF16)
                        for t in range(16)
                    ],
                    axis=1,
                ),
                weights_t[p * T_ROWS : p * T_ROWS + 2048],
                preferred_element_type=F32,
            )
            for h in (0, 1):
                spread[1, h, p, 0:80] = out[80 * h : 80 * h + 80, 0:128]
                spread[0, h, p, 1:81] = out[80 * h : 80 * h + 80, 128:256]

        extras = [blur_halo(p) for p in range(TILES)]
        for p in range(TILES):
            dual(p, extras[p])
        for p in range(TILES):
            adjoint(p)

    for par in (0, 1):
        lay(shifted, par, 8, 72)
    lax.fori_loop(0, TILES, blur_own, 0)
    for p in range(TILES - 1):
        tv(0, p, 0, PAIRS)
        tv(1, p, 0, PAIRS - 8)

    wait_in(0)
    for par in (0, 1):
        for d, (a, b) in ((0, (0, 8)), (1, (72, 80))):
            for p in range(TILES):
                value = masked(d, row_in[0, d, par, p])
                x_e[par, p + 1, a:b] = value
                bar_e[par, p + 1, a:b] = value
            for s, q in ((0, 0), (1, TILES + 1)):
                value = masked(4 + 2 * d + s, unpacked(cor_in[0, 2 * d + s], par, 112 - 112 * s))
                x_e[par, q, a:b] = value
                bar_e[par, q, a:b] = value
        for s, q in ((0, 0), (1, TILES + 1)):
            for k in range(4):
                value = masked(2 + s, unpacked(col_in[0, s], 4 * par + k, 112 - 112 * s))
                x_e[par, q, 8 + 16 * k : 24 + 16 * k] = value
                bar_e[par, q, 8 + 16 * k : 24 + 16 * k] = value
        lay(shifted_halo, par, 0, 8)
        lay(shifted_halo, par, 72, 80)
        lay_sides(par, 8, 72, 0)

    duals(8)
    for p in range(TILES - 1):
        tv(1, p, PAIRS - 8, PAIRS)
    for par in (0, 1):
        tv(par, TILES - 1, 0, PAIRS)

    for par in (0, 1):
        for d, first in ((0, 0), (1, 64)):
            for a, b in ((first, first + 8), (first + 8, first + 16)):
                own = 8 <= a < 72
                tiles = [merged(par, q, a, b) for q in range(TILES + 1)]
                for p in range(TILES):
                    value = own_part(par, p, a, b, tiles) if own else rim_part(par, p, d, tiles)
                    acc[par, p + 1, a:b] = value
                    wide_row_out[d, TILES * par + p, a - first : b - first] = value
                acc[par, 0, a:b] = side_part(par, 0, a, b, tiles[0])
                acc[par, TILES + 1, a:b] = side_part(par, 1, a, b, tiles[TILES])
        a, b = 16, 64
        tiles = [merged(par, q, a, b) if q != 2 else None for q in range(TILES + 1)]
        for p in (0, TILES - 1):
            acc[par, p + 1, a:b] = own_part(par, p, a, b, tiles)
        acc[par, 0, a:b] = side_part(par, 0, a, b, tiles[0])
        acc[par, TILES + 1, a:b] = side_part(par, 1, a, b, tiles[TILES])
    for d, first in ((0, 0), (1, 64)):
        message = None
        for f, (par, s) in enumerate(((0, 0), (0, 1), (1, 0), (1, 1))):
            moved = roll(acc[par, (TILES + 1) * s, first : first + 16], 16 * f - 112 + 112 * s)
            message = moved if f == 0 else jnp.where(lane16 >= 16 * f, moved, message)
        wide_row_out[d, 2 * TILES] = message
    for s, q in ((0, 0), (1, TILES)):
        around = [
            jnp.where(lanes((80, 128)) < 16, roll(acc[par, q], 16), roll(acc[par, q + 1], 16)) for par in (0, 1)
        ]
        message = None
        for f in range(4):
            moved = roll(around[f >> 1][40 * (f & 1) : 40 * (f & 1) + 40], 32 * f)
            message = moved if f == 0 else jnp.where(lanes((40, 128)) >= 32 * f, moved, message)
        wide_col_out[s] = message
        for d, first in ((0, 0), (1, 64)):
            message = None
            for f in range(4):
                start = first + 8 * (f & 1)
                moved = roll(around[f >> 1][start : start + 8], 32 * f)
                message = moved if f == 0 else jnp.where(lane8 >= 32 * f, moved, message)
            wide_cor_out[2 * d + s] = message
    start_out(1)

    for par in (0, 1):
        a, b = 16, 64
        tiles = [None] + [merged(par, q, a, b) for q in (1, 2, 3)] + [None]
        for p in range(TILES):
            value = own_part(par, p, a, b, tiles) if p in (1, 2) else acc[par, p + 1, a:b]
            old = x_e[par, p + 1, a:b]
            new = old - TAU * value
            x_e[par, p + 1, a:b] = new
            bar_e[par, p + 1, a:b] = 2.0 * new - old
        lay(shifted, par, a, b)
        lane = lanes((b - a, 128))
        shifted[par, 0, 0, a:b] = jnp.where(lane < 30, 0.0, shifted[par, 0, 0, a:b])
        shifted[par, 1, TILES - 1, a:b] = jnp.where(lane >= 64, 0.0, shifted[par, 1, TILES - 1, a:b])
        for h in (0, 1):
            for p in range(TILES):
                shifted[par, h, p, 8:16] = jnp.zeros((8, 128), F32)
                shifted[par, h, p, 64:72] = jnp.zeros((8, 128), F32)
    lax.fori_loop(0, TILES, blur_own, 0)
    for p in (1, 2):
        tv(0, p, 8, 56)
        tv(1, p, 8, 48)

    wait_in(1)
    for par in (0, 1):
        beside = []
        for s in (0, 1):
            halves = [masked(2 + s, wide_col_in[s]) for _ in (0, 1)]
            lane = lanes((40, 128))
            low = [jnp.where(lane >= 112, roll(halves[k], 112 - 32 * (2 * par + k)), 0.0) for k in (0, 1)]
            high = [jnp.where(lane < 16, roll(halves[k], -16 - 32 * (2 * par + k)), 0.0) for k in (0, 1)]
            beside.append((jnp.concatenate(low, axis=0), jnp.concatenate(high, axis=0)))
        for a, b in ((16, 64),):
            for s, q in ((0, 0), (1, TILES)):
                for k in (0, 1):
                    more = beside[s][k][a:b]
                    old = x_e[par, q + k, a:b]
                    if q + k in (0, TILES + 1):
                        value = acc[par, q + k, a:b] + more
                        new = old - TAU * value
                        bar_e[par, q + k, a:b] = masked(2 + s, 2.0 * new - old)
                    else:
                        x_e[par, q + k, a:b] = old - TAU * more
                        bar_e[par, q + k, a:b] = bar_e[par, q + k, a:b] - 2.0 * TAU * more
        for d, first in ((0, 0), (1, 64)):
            for k8 in (0, 1):
                a, b = first + 8 * k8, first + 8 * k8 + 8
                for q in range(TILES + 2):
                    value = acc[par, q, a:b]
                    if 1 <= q <= TILES:
                        value = value + masked(d, wide_row_in[d, TILES * par + q - 1, 8 * k8 : 8 * k8 + 8])
                    else:
                        s = 0 if q == 0 else 1
                        f = 2 * par + s
                        more = roll(wide_row_in[d, 2 * TILES, 8 * k8 : 8 * k8 + 8], 112 - 112 * s - 16 * f)
                        value = value + masked(d, jnp.where((lane8 >= 112) if s == 0 else (lane8 < 16), more, 0.0))
                    for s, line in ((0, 0), (1, TILES)):
                        if q in (line, line + 1):
                            message = wide_cor_in[2 * d + s]
                            f = 2 * par + k8
                            if q == line:
                                more = jnp.where(lane8 >= 112, roll(message, 112 - 32 * f), 0.0)
                            else:
                                more = jnp.where(lane8 < 16, roll(message, -16 - 32 * f), 0.0)
                            value = value + beside[s][q - line][a:b] + masked(4 + 2 * d + s, more)
                    old = x_e[par, q, a:b]
                    new = old - TAU * value
                    bar = 2.0 * new - old
                    if q == 0:
                        bar = masked(2, bar)
                    if q == TILES + 1:
                        bar = masked(3, bar)
                    if not 8 <= a < 72:
                        bar = masked(d, bar)
                    x_e[par, q, a:b] = new
                    bar_e[par, q, a:b] = bar
        lay(shifted_halo, par, 0, 16)
        lay(shifted_halo, par, 64, 80)
        lay_sides(par, 16, 64, 15)

    duals(16)
    for p in (1, 2):
        tv(0, p, 0, 8)
        tv(0, p, 56, 64)
        tv(1, p, 0, 8)
        tv(1, p, 48, 64)
    for par in (0, 1):
        for p in (0, TILES - 1):
            tv(par, p, 0, PAIRS)

    corners = [[None, None] for _ in range(4)]
    for par in (0, 1):
        for d, (a, b) in ((0, (0, 8)), (1, (72, 80))):
            tiles = [merged(par, q, a, b) for q in range(TILES + 1)]
            for p in range(TILES):
                row_out[1, d, par, p] = rim_part(par, p, d, tiles)
            for s in (0, 1):
                corners[2 * d + s][par] = side_part(par, s, a, b, tiles[TILES * s])
    for s, first_lane in ((0, 112), (1, 0)):
        side = [side_part(par, s, 8, 72, merged(par, TILES * s, 8, 72)) for par in (0, 1)]
        col_out[1, s] = packed([side[par][16 * k : 16 * k + 16] for par in (0, 1) for k in range(4)], first_lane, 16)
        for d in (0, 1):
            cor_out[1, 2 * d + s] = packed(corners[2 * d + s], first_lane, 8)
    start_out(2)

    for par in (0, 1):
        tiles = [merged(par, q, 8, 72) for q in range(TILES + 1)]
        for p in range(TILES):
            x_e[par, p + 1, 8:72] = x_e[par, p + 1, 8:72] - TAU * own_part(par, p, 8, 72, tiles)
            dual_out_ref[p, pl.ds(par, PAIRS, stride=2), :] = y_v[par, p]

    wait_in(2)

    def subtract(par, q, a, b, value):
        x_e[par, q, a:b] = x_e[par, q, a:b] - TAU * value

    for par in (0, 1):
        for s, q, first_lane in ((0, 1, 0), (1, TILES, 112)):
            message = masked(2 + s, col_in[1, s])
            keep = lane16 < 15 if s == 0 else lane16 >= 113
            for k in range(4):
                value = jnp.where(keep, unpacked(message, 4 * par + k, first_lane), 0.0)
                subtract(par, q, 8 + 16 * k, 24 + 16 * k, value)
        for d, (a, b) in ((0, (8, 16)), (1, (64, 72))):
            for p in range(TILES):
                value = masked(d, row_in[1, d, par, p])
                if p in (0, TILES - 1):
                    s = 0 if p == 0 else 1
                    message = masked(4 + 2 * d + s, cor_in[1, 2 * d + s])
                    keep = lane8 < 15 if s == 0 else lane8 >= 113
                    value = value + jnp.where(keep, unpacked(message, par, 112 * s), 0.0)
                subtract(par, p + 1, a, b, value)
    for par in (0, 1):
        for p in range(TILES):
            restored_ref[p, pl.ds(par, PAIRS, stride=2), :] = x_e[par, p + 1, 8:72]
    for exchange in range(EXCHANGES):
        wait_out(exchange)


def put_out(restored_ref, dual_ref, restored_hbm, dual_hbm, store_sem):
    stores = [
        pltpu.make_async_copy(src.at[p], dst.at[:, 128 * p : 128 * p + 128], store_sem.at[TILES * i + p])
        for i, (src, dst) in enumerate(((restored_ref, restored_hbm), (dual_ref, dual_hbm)))
        for p in range(TILES)
    ]
    for store in stores:
        store.start()
    for store in stores:
        store.wait()


def per_device(observed, psf_table, psf_index, start_image, blur_dual, tv_dual):
    shape = observed.shape
    block = (2, TILES, PAIRS, 128)
    extended = (2, TILES + 2, 80, 128)
    tiled = (TILES, 2 * PAIRS, 128)
    hbm = pl.BlockSpec(memory_space=pl.ANY)
    table = psf_table.transpose(1, 2, 0)
    results = pl.pallas_call(
        kernel,
        out_shape=(pltpu.VMEM(tiled, F32), pltpu.VMEM(tiled, F32)),
        in_specs=[hbm] * 6,
        out_specs=(pl.BlockSpec(memory_space=pltpu.VMEM),) * 2,
        scratch_shapes=[
            pltpu.VMEM(tiled, F32),
            pltpu.VMEM(table.shape, BF16),
            pltpu.SMEM(psf_index.shape, jnp.int32),
            pltpu.VMEM(tiled, F32),
            pltpu.VMEM(tiled, F32),
            pltpu.VMEM((2,) + tiled, F32),
            pltpu.VMEM((8, 64, 128), F32),
            pltpu.VMEM((TILES * 4096, 128), BF16),
            pltpu.VMEM((TILES * T_ROWS, 256), BF16),
            pltpu.VMEM(extended, F32),
            pltpu.VMEM(extended, F32),
            pltpu.VMEM(extended, F32),
            pltpu.VMEM(block, F32),
            pltpu.VMEM(block, F32),
            pltpu.VMEM(block, F32),
            pltpu.VMEM(block, F32),
            pltpu.VMEM((2, 2, TILES, 80, 128), F32),
            pltpu.VMEM((2, 2, TILES, 80, 128), F32),
            pltpu.VMEM((TILES, 128, 128), F32),
            pltpu.VMEM((2, TILES, 96, 128), F32),
            pltpu.VMEM((2, 2, TILES, 88, 128), F32),
            pltpu.VMEM((2, 2, 2, TILES, 8, 128), F32),
            pltpu.VMEM((2, 2, 16, 128), F32),
            pltpu.VMEM((2, 4, 8, 128), F32),
            pltpu.VMEM((2, 2, 2, TILES, 8, 128), F32),
            pltpu.VMEM((2, 2, 16, 128), F32),
            pltpu.VMEM((2, 4, 8, 128), F32),
            pltpu.VMEM((2, 2 * TILES + 1, 16, 128), F32),
            pltpu.VMEM((2, 40, 128), F32),
            pltpu.VMEM((4, 8, 128), F32),
            pltpu.VMEM((2, 2 * TILES + 1, 16, 128), F32),
            pltpu.VMEM((2, 40, 128), F32),
            pltpu.VMEM((4, 8, 128), F32),
            pltpu.SemaphoreType.DMA((4 * TILES + 2,)),
            pltpu.SemaphoreType.DMA((EXCHANGES, 8)),
            pltpu.SemaphoreType.DMA((EXCHANGES, 8)),
        ],
        compiler_params=pltpu.CompilerParams(collective_id=0, has_side_effects=True),
    )(psf_index, observed, table, start_image, blur_dual, tv_dual)
    return pl.pallas_call(
        put_out,
        out_shape=(jax.ShapeDtypeStruct(shape, F32), jax.ShapeDtypeStruct(shape, F32)),
        in_specs=[hbm] * 2,
        out_specs=(hbm, hbm),
        scratch_shapes=[pltpu.SemaphoreType.DMA((2 * TILES,))],
    )(*(pltpu.with_memory_space_constraint(result, pltpu.VMEM) for result in results))


def solution(mesh):
    placed = (
        P("row", "col"),
        P(),
        P("row", "col"),
        P("row", "col"),
        P("row", "col"),
        P(None, "row", "col"),
    )
    return jax.shard_map(
        per_device,
        mesh=mesh,
        in_specs=placed,
        out_specs=(P("row", "col"), P("row", "col")),
        check_vma=False,
    )
```

```python
import jax
import jax.numpy as jnp
from jax import lax
from jax.experimental import pallas as pl
from jax.experimental.pallas import tpu as pltpu
from jax.sharding import PartitionSpec as P

EXCHANGES = 3
SIGMA = 0.15
TAU = 0.6
WEIGHT = 0.5
TAPS = 31
PAIRS = 64
TILES = 4
DIRS = ((-1, 0), (1, 0), (0, -1), (0, 1), (-1, -1), (-1, 1), (1, -1), (1, 1))
OPPOSITE = (1, 0, 3, 2, 7, 6, 5, 4)
MESH_ID = pl.DeviceIdType.MESH
F32 = jnp.float32
BF16 = jnp.bfloat16
STRIP_TYPE = BF16


def lanes(shape):
    return lax.broadcasted_iota(jnp.int32, shape, 1)


def roll(value, shift):
    shift = shift % 128
    return value if shift == 0 else pltpu.roll(value, shift, 1)


T_ROWS = 17 * 128


def kernel(
    index_hbm, observed_hbm, table_hbm, start_hbm, dual_hbm, tv_hbm,
    restored_ref, dual_out_ref,
    start_v, table_v, index_ref, observed_v, dual_v, tv_v,
    base_v, weights, weights_t, x_e, bar_e, acc, obs_v, y_v, q1_v, q2_v, shifted, shifted_halo, blur_v, ypad, spread,
    row_out, col_out, cor_out, row_in, col_in, cor_in,
    wide_row_out, wide_col_out, wide_cor_out, wide_row_in, wide_col_in, wide_cor_in,
    last_row_out, last_row_in,
    load_sem, send_sem, recv_sem,
):
    row, col = lax.axis_index("row"), lax.axis_index("col")
    rows, cols = lax.axis_size("row"), lax.axis_size("col")

    def at(direction):
        dr, dc = direction
        return (lax.rem(row + dr + rows, rows), lax.rem(col + dc + cols, cols))

    top, bottom = row == 0, row == rows - 1
    left, right = col == 0, col == cols - 1
    outside = (top, bottom, left, right, top | left, top | right, bottom | left, bottom | right)
    inside = [jnp.logical_not(o) for o in outside]

    slices = [slice(128 * p, 128 * p + 128) for p in range(TILES)]
    plain = ((start_hbm, start_v), (observed_hbm, observed_v), (dual_hbm, dual_v))
    sources = [(src.at[:, slices[p]], dst.at[p]) for src, dst in plain for p in range(TILES)]
    sources += [(tv_hbm.at[:, :, slices[p]], tv_v.at[:, p]) for p in range(TILES)]
    sources[TILES:TILES] = [(table_hbm, table_v), (index_hbm, index_ref)]
    loads = [pltpu.make_async_copy(src, dst, load_sem.at[i]) for i, (src, dst) in enumerate(sources)]
    for load in loads[:TILES]:
        load.start()

    barrier = pltpu.get_barrier_semaphore()
    for d, direction in enumerate(DIRS):
        @pl.when(inside[d])
        def _():
            pl.semaphore_signal(barrier, inc=1, device_id=at(direction), device_id_type=MESH_ID)

    for load in loads[TILES:]:
        load.start()

    lane64 = lanes((PAIRS, 128))
    lane8 = lanes((8, 128))
    lane16 = lanes((16, 128))

    sides = (col_out, cor_out, col_in, cor_in)
    first_refs = (row_out,) + tuple(ref.at[0] for ref in sides[:2]) + (row_in,) + tuple(ref.at[0] for ref in sides[2:])
    last_refs = (last_row_out,) + tuple(ref.at[1] for ref in sides[:2])
    last_refs += (last_row_in,) + tuple(ref.at[1] for ref in sides[2:])
    wide_refs = (wide_row_out, wide_col_out, wide_cor_out, wide_row_in, wide_col_in, wide_cor_in)

    def copies(exchange):
        refs = (first_refs, wide_refs, last_refs)[exchange]
        result = []
        for d, direction in enumerate(DIRS):
            if d < 2:
                src, dst = refs[0].at[d], refs[3].at[d ^ 1]
            elif d < 4:
                src, dst = refs[1].at[d - 2], refs[4].at[(d - 2) ^ 1]
            else:
                src, dst = refs[2].at[d - 4], refs[5].at[3 - (d - 4)]
            back = OPPOSITE[d]
            result.append(
                pltpu.make_async_remote_copy(
                    src_ref=src,
                    dst_ref=dst,
                    send_sem=send_sem.at[exchange, d],
                    recv_sem=recv_sem.at[exchange, back],
                    device_id=at(direction),
                    device_id_type=MESH_ID,
                )
            )
        return result

    def start_out(exchange):
        for d, copy in enumerate(copies(exchange)):
            pl.when(inside[d])(copy.start)

    def wait_in(exchange):
        for d, copy in enumerate(copies(exchange)):
            pl.when(inside[OPPOSITE[d]])(copy.wait_recv)

    def wait_out(exchange):
        for d, copy in enumerate(copies(exchange)):
            pl.when(inside[d])(copy.wait_send)

    def packed(parts, first_lane, height):
        lane = lane16 if height == 16 else lane8
        message = None
        for f, part in enumerate(parts):
            moved = roll(part, 16 * f - first_lane)
            message = moved if f == 0 else jnp.where(lane >= 16 * f, moved, message)
        return message

    def unpacked(message, f, first_lane):
        return roll(message, first_lane - 16 * f)

    for load in loads[:TILES]:
        load.wait()
    for par in (0, 1):
        for p in range(TILES):
            value = start_v[p, pl.ds(par, PAIRS, stride=2), :]
            x_e[par, p + 1, 8:72] = value
            bar_e[par, p + 1, 8:72] = value
    for d, first in ((0, 8), (1, 64)):
        for par in (0, 1):
            for p in range(TILES):
                row_out[d, par, p] = bar_e[par, p + 1, first : first + 8]
    for s, (q, first_lane) in enumerate(((1, 0), (TILES, 112))):
        col_out[0, s] = packed(
            [bar_e[par, q, 8 + 16 * k : 24 + 16 * k] for par in (0, 1) for k in range(4)], first_lane, 16
        )
        for d, first in ((0, 8), (1, 64)):
            cor_out[0, 2 * d + s] = packed([bar_e[par, q, first : first + 8] for par in (0, 1)], first_lane, 8)

    pl.semaphore_wait(barrier, sum(i.astype(jnp.int32) for i in inside))
    start_out(0)
    for ref in (x_e, bar_e):
        for par in (0, 1):
            for q in range(TILES + 2):
                if q in (0, TILES + 1):
                    ref[par, q] = jnp.zeros((80, 128), F32)
                else:
                    ref[par, q, 0:8] = jnp.zeros((8, 128), F32)
                    ref[par, q, 72:80] = jnp.zeros((8, 128), F32)

    for load in loads[TILES : TILES + 2]:
        load.wait()
    which = lax.broadcasted_iota(jnp.int32, (8, 64), 0) & 3
    entry = lanes((8, 64))
    chosen = jnp.zeros((8, 64), F32)
    for p in range(TILES):
        chosen = jnp.where((which == p) & (entry == index_ref[0, p]), 1.0, chosen)
    chosen = chosen.astype(BF16)
    gap = jnp.zeros((1, 64), F32)
    lines = [
        jnp.concatenate([table_v[a].astype(F32), gap], axis=0).astype(BF16)
        if a < TAPS else jnp.zeros((32, 64), BF16)
        for a in range(32)
    ]
    picked = jnp.concatenate(
        [
            lax.dot_general(
                chosen,
                jnp.concatenate(lines[8 * k : 8 * k + 8], axis=0),
                (((1,), (1,)), ((), ())),
                preferred_element_type=F32,
            )
            for k in range(4)
        ],
        axis=1,
    )
    normed = picked / jnp.sum(picked, axis=1, keepdims=True)
    kernels = jnp.concatenate([normed[:, 128 * q : 128 * q + 128] for q in range(8)], axis=0)
    before = jnp.concatenate([jnp.zeros((8, 128), F32), kernels[:56]], axis=0)
    kernels, before = kernels.astype(BF16), before.astype(BF16)
    tap = lax.broadcasted_iota(jnp.int32, (128, 128), 0)
    place = lanes((128, 128))

    def flip(r, first):
        hit = ((tap >> 5) == r) & (place == ((first - (tap & 31)) & 127))
        return hit.astype(F32).astype(BF16)

    lane_of = lanes((64, 128))
    for r in range(4):
        low = jnp.dot(kernels, flip(r, 128), preferred_element_type=F32)
        high = jnp.dot(kernels if r else before, flip((r - 1) & 3, 64), preferred_element_type=F32)
        base_v[r] = low + high
        base_v[4 + r] = jnp.where(lane_of < 32, roll(kernels.astype(F32), -32 * r), 0.0)
    reach = tap - (place & 63)
    band = (reach >= 0) & (reach < TAPS)
    for p in range(TILES):
        weights_t[p * T_ROWS + 64 : p * T_ROWS + 128, 0:128] = jnp.zeros((64, 128), BF16)

    nothing = jnp.zeros((32, 128), BF16)

    def build(q, carry):
        for p in range(TILES):
            for r in range(4):
                line = base_v[r, pl.ds(q * 8 + p, 1), :]
                rolled = pltpu.roll(jnp.broadcast_to(line, (96, 128)), 0, 1, stride=1, stride_axis=0)
                start = pl.multiple_of(p * 4096 + (q * 4 + r) * 128, 128)
                weights[pl.ds(start, 96), :] = jnp.where(band[:96], rolled, 0.0).astype(BF16)
                weights[pl.ds(start + 96, 32), :] = nothing
                line = base_v[4 + r, pl.ds(q * 8 + p, 1), :]
                rolled = pltpu.roll(jnp.broadcast_to(line, (64, 128)), 0, 1, stride=1, stride_axis=0).astype(BF16)
                for d in (0, 1):
                    t, e = (r + d) >> 1, (r + d) & 1
                    start = pl.multiple_of(p * T_ROWS + (q * 2 + t) * 128 + d * 64, 64)
                    weights_t[pl.ds(start, 64), 128 * e : 128 * e + 128] = rolled
        return carry

    lax.fori_loop(0, 8, build, 0)

    ypad[...] = jnp.zeros_like(ypad)
    shifted[...] = jnp.zeros_like(shifted)
    shifted_halo[...] = jnp.zeros_like(shifted_halo)
    for h in (0, 1):
        for p in range(TILES):
            spread[0, h, p, 0:8] = jnp.zeros((8, 128), F32)
    for load in loads[TILES + 2 :]:
        load.wait()
    for par in (0, 1):
        for p in range(TILES):
            rows_of = pl.ds(par, PAIRS, stride=2)
            obs_v[par, p] = observed_v[p, rows_of, :]
            y_v[par, p] = dual_v[p, rows_of, :]
            q1_v[par, p] = tv_v[0, p, rows_of, :]
            q2_v[par, p] = tv_v[1, p, rows_of, :]

    def stacked_rows(source, p, ranges):
        pieces = []
        for t in range(16):
            for par in (1, 0):
                first = t + 1 - par
                pieces.append(
                    jnp.concatenate(
                        [source[par, h, p, a + first : a + first + n] for h, a, n in ranges], axis=0
                    ).astype(BF16)
                )
        return jnp.concatenate(pieces, axis=1)

    def lay(target, par, a, b):
        lane = lanes((b - a, 128))
        tiles = [bar_e[par, q, a:b] for q in range(TILES + 2)]
        by15 = [roll(t, 15) for t in tiles[:-1]]
        by79 = [roll(t, 79) for t in tiles[1:]]
        for p in range(TILES):
            target[par, 0, p, a:b] = jnp.where(lane < 15, by15[p], by15[p + 1])
            target[par, 1, p, a:b] = jnp.where(lane < 79, by79[p], by79[p + 1])

    def lay_sides(par, a, b, reach_in):
        lane = lanes((b - a, 128))
        first = jnp.where(lane < 15, roll(bar_e[par, 0, a:b], 15), roll(bar_e[par, 1, a:b], 15))
        last = jnp.where(lane < 79, roll(bar_e[par, TILES, a:b], 79), roll(bar_e[par, TILES + 1, a:b], 79))
        shifted_halo[par, 0, 0, a:b] = jnp.where(lane < 15 + reach_in, first, 0.0)
        shifted_halo[par, 1, TILES - 1, a:b] = jnp.where(lane >= 79 - reach_in, last, 0.0)

    def blur_own(p, carry):
        lhs = stacked_rows(shifted, p, ((0, 0, PAIRS), (1, 0, PAIRS)))
        start = p * 4096 if isinstance(p, int) else pl.multiple_of(p * 4096, 4096)
        matrix = weights[pl.ds(start, 4096), :]
        blur_v[p] = jnp.dot(lhs, matrix, preferred_element_type=F32)
        return carry

    def tv(par, p, a, b):
        value = bar_e[par, p + 1, a + 8 : b + 8]
        if par == 0:
            grad1 = bar_e[1, p + 1, a + 8 : b + 8] - value
        else:
            grad1 = bar_e[0, p + 1, a + 9 : b + 9] - value
            if b == PAIRS:
                grad1 = jnp.where(
                    (lax.broadcasted_iota(jnp.int32, (b - a, 128), 0) == b - a - 1) & bottom, 0.0, grad1
                )
        lane = lanes((b - a, 128))
        grad2 = jnp.where(lane < 127, roll(value, 127), roll(bar_e[par, p + 2, a + 8 : b + 8], 127)) - value
        if p + 1 == TILES:
            grad2 = jnp.where((lane == 127) & right, 0.0, grad2)
        u1 = q1_v[par, p, a:b] + SIGMA * grad1
        u2 = q2_v[par, p, a:b] + SIGMA * grad2
        shrink = jnp.maximum(1.0, jnp.sqrt(u1 * u1 + u2 * u2) / WEIGHT)
        q1_v[par, p, a:b] = u1 / shrink
        q2_v[par, p, a:b] = u2 / shrink

    def moved_tiles(par, a, b, wanted):
        firsts = [roll(spread[par, 0, p, a:b], 113) if wanted(p - 1) or wanted(p) else None for p in range(TILES)]
        seconds = [roll(spread[par, 1, p, a:b], 49) if wanted(p) or wanted(p + 1) else None for p in range(TILES)]
        return firsts + [0.0], [0.0] + seconds

    def merged(p, tiles, rows_count):
        firsts, seconds = tiles
        lane = lanes((rows_count, 128))
        if p == -1:
            return jnp.where(lane >= 113, firsts[0], 0.0)
        if p == TILES:
            return jnp.where(lane < 15, seconds[TILES], 0.0)
        return jnp.where(lane < 113, firsts[p], firsts[p + 1]) + jnp.where(lane >= 49, seconds[p + 1], seconds[p])

    def own_part(par, p, a, b, tiles):
        lane = lanes((b - a, 128))
        sub = lax.broadcasted_iota(jnp.int32, (b - a, 128), 0)
        i, j = a - 8, b - 8
        m1, m2 = q1_v[par, p, i:j], q2_v[par, p, i:j]
        if par == 1:
            above = q1_v[0, p, i:j]
            if b == 72:
                m1 = jnp.where((sub == b - a - 1) & bottom, 0.0, m1)
        elif a == 8:
            above = jnp.concatenate([jnp.zeros((1, 128), F32), q1_v[1, p, : j - 1]], axis=0)
        else:
            above = q1_v[1, p, i - 1 : j - 1]
        outer = roll(q2_v[par, p - 1, i:j], 1) if p else 0.0
        before = jnp.where(lane == 0, outer, roll(m2, 1))
        if p + 1 == TILES:
            m2 = jnp.where((lane == 127) & right, 0.0, m2)
        return merged(p, tiles, b - a) - ((m1 - above) + (m2 - before))

    def rim_part(par, p, d, tiles):
        value = merged(p, tiles, 8)
        if d == 1 and par == 0:
            edge = jnp.concatenate([q1_v[1, p, PAIRS - 1 : PAIRS], jnp.zeros((7, 128), F32)], axis=0)
            value = value + edge
        return value

    def side_part(par, s, a, b, tiles):
        value = merged(TILES if s else -1, tiles, b - a)
        if s == 1 and 8 <= a < 72:
            edge = roll(q2_v[par, TILES - 1, a - 8 : b - 8], 1)
            value = value + jnp.where(lanes((b - a, 128)) == 0, edge, 0.0)
        return value

    def masked(direction, value):
        return jnp.where(outside[direction], 0.0, value)

    def duals(edge):
        gap = jnp.zeros((PAIRS - 2 * edge, 128), F32)

        def rows_full(p):
            return 0 if p == 0 else 1 if p + 1 == TILES else None

        def blur_halo(p):
            full = rows_full(p)
            ranges = [(full, 0, PAIRS)] if full is not None else []
            for h in (0, 1):
                if h != full:
                    ranges += [(h, 0, edge), (h, PAIRS - edge, edge)]
            return jnp.dot(
                stacked_rows(shifted_halo, p, ranges),
                weights[p * 4096 : p * 4096 + 4096],
                preferred_element_type=F32,
            )

        def dual(p, extra):
            full = rows_full(p)
            halves, place_r = [None, None], 0
            if full is not None:
                halves[full] = blur_v[p, PAIRS * full : PAIRS * full + PAIRS] + extra[:PAIRS]
                place_r = PAIRS
            for h in (0, 1):
                if h != full:
                    more = jnp.concatenate(
                        [extra[place_r : place_r + edge], gap, extra[place_r + edge : place_r + 2 * edge]], axis=0
                    )
                    halves[h] = blur_v[p, PAIRS * h : PAIRS * h + PAIRS] + more
                    place_r += 2 * edge
            even = jnp.where(lane64 < 64, halves[0], roll(halves[1], 64))
            odd = jnp.where(lane64 < 64, roll(halves[0], 64), halves[1])
            new = []
            for par, value in ((0, even), (1, odd)):
                updated = (y_v[par, p] + SIGMA * (value - obs_v[par, p])) / (1.0 + SIGMA)
                y_v[par, p] = updated
                new.append(updated)
            ypad[0, p, 16 : 16 + PAIRS] = jnp.where(lane64 < 64, new[0], roll(new[1], 64))
            ypad[1, p, 16 : 16 + PAIRS] = jnp.where(lane64 < 64, roll(new[0], 64), new[1])

        def adjoint(p):
            out = jnp.dot(
                jnp.concatenate(
                    [
                        jnp.concatenate([ypad[h, p, 16 - t : 96 - t] for h in (0, 1)], axis=0).astype(BF16)
                        for t in range(16)
                    ],
                    axis=1,
                ),
                weights_t[p * T_ROWS : p * T_ROWS + 2048],
                preferred_element_type=F32,
            )
            for h in (0, 1):
                spread[1, h, p, 0:80] = out[80 * h : 80 * h + 80, 0:128]
                spread[0, h, p, 1:81] = out[80 * h : 80 * h + 80, 128:256]

        order = (0, 1, 2, 3)
        extras = {p: blur_halo(p) for p in order}
        for p in order:
            dual(p, extras[p])
        for p in (0, 1, 2, 3):
            adjoint(p)

    for par in (0, 1):
        lay(shifted, par, 8, 72)
    for p in range(TILES):
        blur_own(p, 0)
    for p in range(TILES - 1):
        tv(0, p, 0, PAIRS)
        tv(1, p, 0, PAIRS - 8)

    wait_in(0)
    for par in (0, 1):
        for d, (a, b) in ((0, (0, 8)), (1, (72, 80))):
            for p in range(TILES):
                value = masked(d, row_in[d, par, p])
                x_e[par, p + 1, a:b] = value
                bar_e[par, p + 1, a:b] = value
            for s, q in ((0, 0), (1, TILES + 1)):
                value = masked(4 + 2 * d + s, unpacked(cor_in[0, 2 * d + s], par, 112 - 112 * s))
                x_e[par, q, a:b] = value
                bar_e[par, q, a:b] = value
        for s, q in ((0, 0), (1, TILES + 1)):
            for k in range(4):
                value = masked(2 + s, unpacked(col_in[0, s], 4 * par + k, 112 - 112 * s))
                x_e[par, q, 8 + 16 * k : 24 + 16 * k] = value
                bar_e[par, q, 8 + 16 * k : 24 + 16 * k] = value
        lay(shifted_halo, par, 0, 8)
        lay(shifted_halo, par, 72, 80)
        lay_sides(par, 8, 72, 0)

    duals(8)
    for p in range(TILES - 1):
        tv(1, p, PAIRS - 8, PAIRS)
    for par in (0, 1):
        tv(par, TILES - 1, 0, PAIRS)

    every = lambda p: True
    for par in (0, 1):
        for d, first in ((0, 0), (1, 64)):
            strip = [[], [], [], []]
            for a, b in ((first, first + 8), (first + 8, first + 16)):
                own = 8 <= a < 72
                tiles = moved_tiles(par, a, b, every)
                for p in range(TILES):
                    value = own_part(par, p, a, b, tiles) if own else rim_part(par, p, d, tiles)
                    acc[par, p + 1, a:b] = value
                    strip[p].append(value)
                acc[par, 0, a:b] = side_part(par, 0, a, b, tiles)
                acc[par, TILES + 1, a:b] = side_part(par, 1, a, b, tiles)
            for p in range(TILES):
                wide_row_out[d, TILES * par + p] = jnp.concatenate(strip[p], axis=0).astype(STRIP_TYPE)
        a, b = 16, 64
        tiles = moved_tiles(par, a, b, lambda p: p not in (1, 2))
        for p in (0, TILES - 1):
            acc[par, p + 1, a:b] = own_part(par, p, a, b, tiles)
        acc[par, 0, a:b] = side_part(par, 0, a, b, tiles)
        acc[par, TILES + 1, a:b] = side_part(par, 1, a, b, tiles)
    for d, first in ((0, 0), (1, 64)):
        message = None
        for f, (par, s) in enumerate(((0, 0), (0, 1), (1, 0), (1, 1))):
            moved = roll(acc[par, (TILES + 1) * s, first : first + 16], 16 * f - 112 + 112 * s)
            message = moved if f == 0 else jnp.where(lane16 >= 16 * f, moved, message)
        wide_row_out[d, 2 * TILES] = message.astype(STRIP_TYPE)
    for s, q in ((0, 0), (1, TILES)):
        around = [
            jnp.where(lanes((80, 128)) < 16, roll(acc[par, q], 16), roll(acc[par, q + 1], 16)) for par in (0, 1)
        ]
        message = None
        for f in range(4):
            moved = roll(around[f >> 1][40 * (f & 1) : 40 * (f & 1) + 40], 32 * f)
            message = moved if f == 0 else jnp.where(lanes((40, 128)) >= 32 * f, moved, message)
        wide_col_out[s] = message
        for d, first in ((0, 0), (1, 64)):
            message = None
            for f in range(4):
                start = first + 8 * (f & 1)
                moved = roll(around[f >> 1][start : start + 8], 32 * f)
                message = moved if f == 0 else jnp.where(lane8 >= 32 * f, moved, message)
            wide_cor_out[2 * d + s] = message
    start_out(1)

    for par in (0, 1):
        a, b = 16, 64
        tiles = moved_tiles(par, a, b, lambda p: p in (1, 2))
        for p in range(TILES):
            value = own_part(par, p, a, b, tiles) if p in (1, 2) else acc[par, p + 1, a:b]
            old = x_e[par, p + 1, a:b]
            new = old - TAU * value
            x_e[par, p + 1, a:b] = new
            bar_e[par, p + 1, a:b] = 2.0 * new - old
        lay(shifted, par, a, b)
        lane = lanes((b - a, 128))
        shifted[par, 0, 0, a:b] = jnp.where(lane < 30, 0.0, shifted[par, 0, 0, a:b])
        shifted[par, 1, TILES - 1, a:b] = jnp.where(lane >= 64, 0.0, shifted[par, 1, TILES - 1, a:b])
        for h in (0, 1):
            for p in range(TILES):
                shifted[par, h, p, 8:16] = jnp.zeros((8, 128), F32)
                shifted[par, h, p, 64:72] = jnp.zeros((8, 128), F32)
    lax.fori_loop(0, TILES, blur_own, 0)
    for p in (1, 2):
        tv(0, p, 8, 56)
        tv(1, p, 8, 48)

    wait_in(1)
    strips = [[wide_row_in[d, i].astype(F32) for i in range(2 * TILES + 1)] for d in (0, 1)]
    for par in (0, 1):
        beside = []
        for s in (0, 1):
            halves = [masked(2 + s, wide_col_in[s]) for _ in (0, 1)]
            lane = lanes((40, 128))
            low = [jnp.where(lane >= 112, roll(halves[k], 112 - 32 * (2 * par + k)), 0.0) for k in (0, 1)]
            high = [jnp.where(lane < 16, roll(halves[k], -16 - 32 * (2 * par + k)), 0.0) for k in (0, 1)]
            beside.append((jnp.concatenate(low, axis=0), jnp.concatenate(high, axis=0)))
        for a, b in ((16, 64),):
            for s, q in ((0, 0), (1, TILES)):
                for k in (0, 1):
                    more = beside[s][k][a:b]
                    old = x_e[par, q + k, a:b]
                    if q + k in (0, TILES + 1):
                        value = acc[par, q + k, a:b] + more
                        new = old - TAU * value
                        bar_e[par, q + k, a:b] = masked(2 + s, 2.0 * new - old)
                    else:
                        x_e[par, q + k, a:b] = old - TAU * more
                        bar_e[par, q + k, a:b] = bar_e[par, q + k, a:b] - 2.0 * TAU * more
        for d, first in ((0, 0), (1, 64)):
            for k8 in (0, 1):
                a, b = first + 8 * k8, first + 8 * k8 + 8
                for q in range(TILES + 2):
                    value = acc[par, q, a:b]
                    if 1 <= q <= TILES:
                        value = value + masked(d, strips[d][TILES * par + q - 1][8 * k8 : 8 * k8 + 8])
                    else:
                        s = 0 if q == 0 else 1
                        f = 2 * par + s
                        more = roll(strips[d][2 * TILES][8 * k8 : 8 * k8 + 8], 112 - 112 * s - 16 * f)
                        value = value + masked(d, jnp.where((lane8 >= 112) if s == 0 else (lane8 < 16), more, 0.0))
                    for s, line in ((0, 0), (1, TILES)):
                        if q in (line, line + 1):
                            message = wide_cor_in[2 * d + s]
                            f = 2 * par + k8
                            if q == line:
                                more = jnp.where(lane8 >= 112, roll(message, 112 - 32 * f), 0.0)
                            else:
                                more = jnp.where(lane8 < 16, roll(message, -16 - 32 * f), 0.0)
                            value = value + beside[s][q - line][a:b] + masked(4 + 2 * d + s, more)
                    old = x_e[par, q, a:b]
                    new = old - TAU * value
                    bar = 2.0 * new - old
                    if q == 0:
                        bar = masked(2, bar)
                    if q == TILES + 1:
                        bar = masked(3, bar)
                    if not 8 <= a < 72:
                        bar = masked(d, bar)
                    x_e[par, q, a:b] = new
                    bar_e[par, q, a:b] = bar
        lay(shifted_halo, par, 0, 16)
        lay(shifted_halo, par, 64, 80)
        lay_sides(par, 16, 64, 15)

    duals(16)
    for p in (1, 2):
        tv(0, p, 0, 8)
        tv(0, p, 56, 64)
        tv(1, p, 0, 8)
        tv(1, p, 48, 64)
    for par in (0, 1):
        for p in (0, TILES - 1):
            tv(par, p, 0, PAIRS)

    corners = [[None, None] for _ in range(4)]
    strip = [[[], [], [], []] for _ in (0, 1)]
    for par in (0, 1):
        for d, (a, b) in ((0, (0, 8)), (1, (72, 80))):
            tiles = moved_tiles(par, a, b, every)
            for p in range(TILES):
                strip[d][p].append(rim_part(par, p, d, tiles))
            for s in (0, 1):
                corners[2 * d + s][par] = side_part(par, s, a, b, tiles)
    for d in (0, 1):
        for p in range(TILES):
            last_row_out[d, p] = jnp.concatenate(strip[d][p], axis=0)
    for s, first_lane in ((0, 112), (1, 0)):
        side = [
            side_part(par, s, 8, 72, moved_tiles(par, 8, 72, lambda p: p == (TILES if s else -1)))
            for par in (0, 1)
        ]
        col_out[1, s] = packed([side[par][16 * k : 16 * k + 16] for par in (0, 1) for k in range(4)], first_lane, 16)
        for d in (0, 1):
            cor_out[1, 2 * d + s] = packed(corners[2 * d + s], first_lane, 8)
    start_out(2)

    for par in (0, 1):
        tiles = moved_tiles(par, 8, 72, every)
        for p in range(TILES):
            x_e[par, p + 1, 8:72] = x_e[par, p + 1, 8:72] - TAU * own_part(par, p, 8, 72, tiles)
            dual_out_ref[p, pl.ds(par, PAIRS, stride=2), :] = y_v[par, p]

    wait_in(2)
    strips = [[last_row_in[d, p] for p in range(TILES)] for d in (0, 1)]

    def subtract(par, q, a, b, value):
        x_e[par, q, a:b] = x_e[par, q, a:b] - TAU * value

    for par in (0, 1):
        for s, q, first_lane in ((0, 1, 0), (1, TILES, 112)):
            message = masked(2 + s, col_in[1, s])
            keep = lane16 < 15 if s == 0 else lane16 >= 113
            for k in range(4):
                value = jnp.where(keep, unpacked(message, 4 * par + k, first_lane), 0.0)
                subtract(par, q, 8 + 16 * k, 24 + 16 * k, value)
        for d, (a, b) in ((0, (8, 16)), (1, (64, 72))):
            for p in range(TILES):
                value = masked(d, strips[d][p][8 * par : 8 * par + 8])
                if p in (0, TILES - 1):
                    s = 0 if p == 0 else 1
                    message = masked(4 + 2 * d + s, cor_in[1, 2 * d + s])
                    keep = lane8 < 15 if s == 0 else lane8 >= 113
                    value = value + jnp.where(keep, unpacked(message, par, 112 * s), 0.0)
                subtract(par, p + 1, a, b, value)
    for par in (0, 1):
        for p in range(TILES):
            restored_ref[p, pl.ds(par, PAIRS, stride=2), :] = x_e[par, p + 1, 8:72]
    for exchange in range(EXCHANGES):
        wait_out(exchange)


def put_out(restored_ref, dual_ref, restored_hbm, dual_hbm, store_sem):
    stores = [
        pltpu.make_async_copy(src.at[p], dst.at[:, 128 * p : 128 * p + 128], store_sem.at[TILES * i + p])
        for i, (src, dst) in enumerate(((restored_ref, restored_hbm), (dual_ref, dual_hbm)))
        for p in range(TILES)
    ]
    for store in stores:
        store.start()
    for store in stores:
        store.wait()


def per_device(observed, psf_table, psf_index, start_image, blur_dual, tv_dual):
    shape = observed.shape
    block = (2, TILES, PAIRS, 128)
    extended = (2, TILES + 2, 80, 128)
    tiled = (TILES, 2 * PAIRS, 128)
    hbm = pl.BlockSpec(memory_space=pl.ANY)
    table = psf_table.transpose(1, 2, 0)
    results = pl.pallas_call(
        kernel,
        out_shape=(pltpu.VMEM(tiled, F32), pltpu.VMEM(tiled, F32)),
        in_specs=[hbm] * 6,
        out_specs=(pl.BlockSpec(memory_space=pltpu.VMEM),) * 2,
        scratch_shapes=[
            pltpu.VMEM(tiled, F32),
            pltpu.VMEM(table.shape, BF16),
            pltpu.SMEM(psf_index.shape, jnp.int32),
            pltpu.VMEM(tiled, F32),
            pltpu.VMEM(tiled, F32),
            pltpu.VMEM((2,) + tiled, F32),
            pltpu.VMEM((8, 64, 128), F32),
            pltpu.VMEM((TILES * 4096, 128), BF16),
            pltpu.VMEM((TILES * T_ROWS, 256), BF16),
            pltpu.VMEM(extended, F32),
            pltpu.VMEM(extended, F32),
            pltpu.VMEM(extended, F32),
            pltpu.VMEM(block, F32),
            pltpu.VMEM(block, F32),
            pltpu.VMEM(block, F32),
            pltpu.VMEM(block, F32),
            pltpu.VMEM((2, 2, TILES, 80, 128), F32),
            pltpu.VMEM((2, 2, TILES, 80, 128), F32),
            pltpu.VMEM((TILES, 128, 128), F32),
            pltpu.VMEM((2, TILES, 96, 128), F32),
            pltpu.VMEM((2, 2, TILES, 88, 128), F32),
            pltpu.VMEM((2, 2, TILES, 8, 128), F32),
            pltpu.VMEM((2, 2, 16, 128), F32),
            pltpu.VMEM((2, 4, 8, 128), F32),
            pltpu.VMEM((2, 2, TILES, 8, 128), F32),
            pltpu.VMEM((2, 2, 16, 128), F32),
            pltpu.VMEM((2, 4, 8, 128), F32),
            pltpu.VMEM((2, 2 * TILES + 1, 16, 128), STRIP_TYPE),
            pltpu.VMEM((2, 40, 128), F32),
            pltpu.VMEM((4, 8, 128), F32),
            pltpu.VMEM((2, 2 * TILES + 1, 16, 128), STRIP_TYPE),
            pltpu.VMEM((2, 40, 128), F32),
            pltpu.VMEM((4, 8, 128), F32),
            pltpu.VMEM((2, TILES, 16, 128), F32),
            pltpu.VMEM((2, TILES, 16, 128), F32),
            pltpu.SemaphoreType.DMA((4 * TILES + 2,)),
            pltpu.SemaphoreType.DMA((EXCHANGES, 8)),
            pltpu.SemaphoreType.DMA((EXCHANGES, 8)),
        ],
        compiler_params=pltpu.CompilerParams(collective_id=0, has_side_effects=True),
    )(psf_index, observed, table, start_image, blur_dual, tv_dual)
    return pl.pallas_call(
        put_out,
        out_shape=(jax.ShapeDtypeStruct(shape, F32), jax.ShapeDtypeStruct(shape, F32)),
        in_specs=[hbm] * 2,
        out_specs=(hbm, hbm),
        scratch_shapes=[pltpu.SemaphoreType.DMA((2 * TILES,))],
    )(*(pltpu.with_memory_space_constraint(result, pltpu.VMEM) for result in results))


def solution(mesh):
    placed = (
        P("row", "col"),
        P(),
        P("row", "col"),
        P("row", "col"),
        P("row", "col"),
        P(None, "row", "col"),
    )
    return jax.shard_map(
        per_device,
        mesh=mesh,
        in_specs=placed,
        out_specs=(P("row", "col"), P("row", "col")),
        check_vma=False,
    )
```

```python
import jax
import jax.numpy as jnp
from jax import lax
from jax.experimental import pallas as pl
from jax.experimental.pallas import tpu as pltpu
from jax.sharding import PartitionSpec as P

EXCHANGES = 3
SIGMA = 0.15
TAU = 0.6
WEIGHT = 0.5
TAPS = 31
PAIRS = 64
TILES = 4
DIRS = ((-1, 0), (1, 0), (0, -1), (0, 1), (-1, -1), (-1, 1), (1, -1), (1, 1))
OPPOSITE = (1, 0, 3, 2, 7, 6, 5, 4)
MESH_ID = pl.DeviceIdType.MESH
F32 = jnp.float32
BF16 = jnp.bfloat16
STRIP_TYPE = BF16


def lanes(shape):
    return lax.broadcasted_iota(jnp.int32, shape, 1)


def roll(value, shift):
    shift = shift % 128
    return value if shift == 0 else pltpu.roll(value, shift, 1)


W_ROWS = 32 * 96
T_ROWS = 17 * 128


def kernel(
    index_hbm, observed_hbm, table_hbm, start_hbm, dual_hbm, tv_hbm,
    restored_ref, dual_out_ref,
    start_v, table_v, index_ref, observed_v, dual_v, tv_v,
    base_v, weights, weights_t, x_e, bar_e, acc, obs_v, y_v, q1_v, q2_v, shifted, shifted_halo, blur_v, ypad, spread,
    row_out, col_out, cor_out, row_in, col_in, cor_in,
    wide_row_out, wide_col_out, wide_cor_out, wide_row_in, wide_col_in, wide_cor_in,
    last_row_out, last_row_in,
    load_sem, send_sem, recv_sem,
):
    row, col = lax.axis_index("row"), lax.axis_index("col")
    rows, cols = lax.axis_size("row"), lax.axis_size("col")

    def at(direction):
        dr, dc = direction
        return (lax.rem(row + dr + rows, rows), lax.rem(col + dc + cols, cols))

    top, bottom = row == 0, row == rows - 1
    left, right = col == 0, col == cols - 1
    outside = (top, bottom, left, right, top | left, top | right, bottom | left, bottom | right)
    inside = [jnp.logical_not(o) for o in outside]

    slices = [slice(128 * p, 128 * p + 128) for p in range(TILES)]
    plain = ((start_hbm, start_v), (observed_hbm, observed_v), (dual_hbm, dual_v))
    sources = [(src.at[:, slices[p]], dst.at[p]) for src, dst in plain for p in range(TILES)]
    sources += [(tv_hbm.at[:, :, slices[p]], tv_v.at[:, p]) for p in range(TILES)]
    sources[TILES:TILES] = [(table_hbm, table_v), (index_hbm, index_ref)]
    loads = [pltpu.make_async_copy(src, dst, load_sem.at[i]) for i, (src, dst) in enumerate(sources)]
    for load in loads[:TILES]:
        load.start()

    barrier = pltpu.get_barrier_semaphore()
    for d, direction in enumerate(DIRS):
        @pl.when(inside[d])
        def _():
            pl.semaphore_signal(barrier, inc=1, device_id=at(direction), device_id_type=MESH_ID)

    for load in loads[TILES:]:
        load.start()

    lane64 = lanes((PAIRS, 128))
    lane8 = lanes((8, 128))
    lane16 = lanes((16, 128))

    sides = (col_out, cor_out, col_in, cor_in)
    first_refs = (row_out,) + tuple(ref.at[0] for ref in sides[:2]) + (row_in,) + tuple(ref.at[0] for ref in sides[2:])
    last_refs = (last_row_out,) + tuple(ref.at[1] for ref in sides[:2])
    last_refs += (last_row_in,) + tuple(ref.at[1] for ref in sides[2:])
    wide_refs = (wide_row_out, wide_col_out, wide_cor_out, wide_row_in, wide_col_in, wide_cor_in)

    def copies(exchange):
        refs = (first_refs, wide_refs, last_refs)[exchange]
        result = []
        for d, direction in enumerate(DIRS):
            if d < 2:
                src, dst = refs[0].at[d], refs[3].at[d ^ 1]
            elif d < 4:
                src, dst = refs[1].at[d - 2], refs[4].at[(d - 2) ^ 1]
            else:
                src, dst = refs[2].at[d - 4], refs[5].at[3 - (d - 4)]
            back = OPPOSITE[d]
            result.append(
                pltpu.make_async_remote_copy(
                    src_ref=src,
                    dst_ref=dst,
                    send_sem=send_sem.at[exchange, d],
                    recv_sem=recv_sem.at[exchange, back],
                    device_id=at(direction),
                    device_id_type=MESH_ID,
                )
            )
        return result

    def start_out(exchange):
        for d, copy in enumerate(copies(exchange)):
            pl.when(inside[d])(copy.start)

    def wait_in(exchange):
        for d, copy in enumerate(copies(exchange)):
            pl.when(inside[OPPOSITE[d]])(copy.wait_recv)

    def wait_out(exchange):
        for d, copy in enumerate(copies(exchange)):
            pl.when(inside[d])(copy.wait_send)

    def packed(parts, first_lane, height):
        lane = lane16 if height == 16 else lane8
        message = None
        for f, part in enumerate(parts):
            moved = roll(part, 16 * f - first_lane)
            message = moved if f == 0 else jnp.where(lane >= 16 * f, moved, message)
        return message

    def unpacked(message, f, first_lane):
        return roll(message, first_lane - 16 * f)

    for load in loads[:TILES]:
        load.wait()
    for par in (0, 1):
        for p in range(TILES):
            value = start_v[p, pl.ds(par, PAIRS, stride=2), :]
            x_e[par, p + 1, 8:72] = value
            bar_e[par, p + 1, 8:72] = value
    for d, first in ((0, 8), (1, 64)):
        for par in (0, 1):
            for p in range(TILES):
                row_out[d, par, p] = bar_e[par, p + 1, first : first + 8]
    for s, (q, first_lane) in enumerate(((1, 0), (TILES, 112))):
        col_out[0, s] = packed(
            [bar_e[par, q, 8 + 16 * k : 24 + 16 * k] for par in (0, 1) for k in range(4)], first_lane, 16
        )
        for d, first in ((0, 8), (1, 64)):
            cor_out[0, 2 * d + s] = packed([bar_e[par, q, first : first + 8] for par in (0, 1)], first_lane, 8)

    pl.semaphore_wait(barrier, sum(i.astype(jnp.int32) for i in inside))
    start_out(0)
    for ref in (x_e, bar_e):
        for par in (0, 1):
            for q in range(TILES + 2):
                if q in (0, TILES + 1):
                    ref[par, q] = jnp.zeros((80, 128), F32)
                else:
                    ref[par, q, 0:8] = jnp.zeros((8, 128), F32)
                    ref[par, q, 72:80] = jnp.zeros((8, 128), F32)

    for load in loads[TILES : TILES + 2]:
        load.wait()
    which = lax.broadcasted_iota(jnp.int32, (8, 64), 0) & 3
    entry = lanes((8, 64))
    chosen = jnp.zeros((8, 64), F32)
    for p in range(TILES):
        chosen = jnp.where((which == p) & (entry == index_ref[0, p]), 1.0, chosen)
    chosen = chosen.astype(BF16)
    gap = jnp.zeros((1, 64), F32)
    lines = [
        jnp.concatenate([table_v[a].astype(F32), gap], axis=0).astype(BF16)
        if a < TAPS else jnp.zeros((32, 64), BF16)
        for a in range(32)
    ]
    picked = jnp.concatenate(
        [
            lax.dot_general(
                chosen,
                jnp.concatenate(lines[8 * k : 8 * k + 8], axis=0),
                (((1,), (1,)), ((), ())),
                preferred_element_type=F32,
            )
            for k in range(4)
        ],
        axis=1,
    )
    normed = picked / jnp.sum(picked, axis=1, keepdims=True)
    kernels = jnp.concatenate([normed[:, 128 * q : 128 * q + 128] for q in range(8)], axis=0)
    before = jnp.concatenate([jnp.zeros((8, 128), F32), kernels[:56]], axis=0)
    kernels, before = kernels.astype(BF16), before.astype(BF16)
    tap = lax.broadcasted_iota(jnp.int32, (128, 128), 0)
    place = lanes((128, 128))

    def flip(r, first):
        hit = ((tap >> 5) == r) & (place == ((first - (tap & 31)) & 127))
        return hit.astype(F32).astype(BF16)

    lane_of = lanes((64, 128))
    for r in range(4):
        low = jnp.dot(kernels, flip(r, 128), preferred_element_type=F32)
        high = jnp.dot(kernels if r else before, flip((r - 1) & 3, 64), preferred_element_type=F32)
        base_v[r] = low + high
        base_v[4 + r] = jnp.where(lane_of < 32, roll(kernels.astype(F32), -32 * r), 0.0)
    reach = tap - (place & 63)
    band = (reach >= 0) & (reach < TAPS)
    for p in range(TILES):
        weights_t[p * T_ROWS + 64 : p * T_ROWS + 128, 0:128] = jnp.zeros((64, 128), BF16)


    def build(q, carry):
        for p in range(TILES):
            for r in range(4):
                line = base_v[r, pl.ds(q * 8 + p, 1), :]
                rolled = pltpu.roll(jnp.broadcast_to(line, (96, 128)), 0, 1, stride=1, stride_axis=0)
                start = pl.multiple_of(p * W_ROWS + (q * 4 + r) * 96, 32)
                weights[pl.ds(start, 96), :] = jnp.where(band[:96], rolled, 0.0).astype(BF16)
                line = base_v[4 + r, pl.ds(q * 8 + p, 1), :]
                rolled = pltpu.roll(jnp.broadcast_to(line, (64, 128)), 0, 1, stride=1, stride_axis=0).astype(BF16)
                for d in (0, 1):
                    t, e = (r + d) >> 1, (r + d) & 1
                    start = pl.multiple_of(p * T_ROWS + (q * 2 + t) * 128 + d * 64, 64)
                    weights_t[pl.ds(start, 64), 128 * e : 128 * e + 128] = rolled
        return carry

    lax.fori_loop(0, 8, build, 0)

    ypad[...] = jnp.zeros_like(ypad)
    shifted[...] = jnp.zeros_like(shifted)
    shifted_halo[...] = jnp.zeros_like(shifted_halo)
    for h in (0, 1):
        for p in range(TILES):
            spread[0, h, p, 0:8] = jnp.zeros((8, 128), F32)
    for load in loads[TILES + 2 :]:
        load.wait()
    for par in (0, 1):
        for p in range(TILES):
            rows_of = pl.ds(par, PAIRS, stride=2)
            obs_v[par, p] = observed_v[p, rows_of, :]
            y_v[par, p] = dual_v[p, rows_of, :]
            q1_v[par, p] = tv_v[0, p, rows_of, :]
            q2_v[par, p] = tv_v[1, p, rows_of, :]

    def stacked_rows(source, p, ranges):
        pieces = []
        for t in range(0, 16, 2):
            parts = []
            for v in (0, 1):
                for par in (1, 0):
                    first = t + v + 1 - par
                    parts.append(
                        jnp.concatenate(
                            [source[par, v, h, p, a + first : a + first + n] for h, a, n in ranges], axis=0
                        )
                    )
            lane = lanes(parts[0].shape)
            for i, border in enumerate((96, 64, 32)):
                pieces.append(jnp.where(lane < border, parts[i], parts[i + 1]).astype(BF16))
        return jnp.concatenate(pieces, axis=1)

    def starts_at(par, v):
        return (96 - 64 * v if par == 0 else 64 * v)

    def beyond(lane, offset, k):
        return ((lane - offset) & 127) >= k

    def lay(target, par, a, b):
        lane = lanes((b - a, 128))
        tiles = [bar_e[par, q, a:b] for q in range(TILES + 2)]
        for v in (0, 1):
            offset = starts_at(par, v)
            by15 = [roll(t, 15 + offset) for t in tiles[:-1]]
            by79 = [roll(t, 79 + offset) for t in tiles[1:]]
            for p in range(TILES):
                target[par, v, 0, p, a:b] = jnp.where(beyond(lane, offset, 15), by15[p + 1], by15[p])
                target[par, v, 1, p, a:b] = jnp.where(beyond(lane, offset, 79), by79[p + 1], by79[p])

    def lay_sides(par, a, b, reach_in):
        lane = lanes((b - a, 128))
        for v in (0, 1):
            offset = starts_at(par, v)
            outer, inner = roll(bar_e[par, 0, a:b], 15 + offset), roll(bar_e[par, 1, a:b], 15 + offset)
            first = jnp.where(beyond(lane, offset, 15), inner, outer)
            inner, outer = roll(bar_e[par, TILES, a:b], 79 + offset), roll(bar_e[par, TILES + 1, a:b], 79 + offset)
            last = jnp.where(beyond(lane, offset, 79), outer, inner)
            shifted_halo[par, v, 0, 0, a:b] = jnp.where(beyond(lane, offset, 15 + reach_in), 0.0, first)
            shifted_halo[par, v, 1, TILES - 1, a:b] = jnp.where(beyond(lane, offset, 79 - reach_in), last, 0.0)

    def blur_own(p, carry):
        lhs = stacked_rows(shifted, p, ((0, 0, PAIRS), (1, 0, PAIRS)))
        start = p * W_ROWS if isinstance(p, int) else pl.multiple_of(p * W_ROWS, W_ROWS)
        matrix = weights[pl.ds(start, W_ROWS), :]
        blur_v[p] = jnp.dot(lhs, matrix, preferred_element_type=F32)
        return carry

    def tv(par, p, a, b):
        value = bar_e[par, p + 1, a + 8 : b + 8]
        if par == 0:
            grad1 = bar_e[1, p + 1, a + 8 : b + 8] - value
        else:
            grad1 = bar_e[0, p + 1, a + 9 : b + 9] - value
            if b == PAIRS:
                grad1 = jnp.where(
                    (lax.broadcasted_iota(jnp.int32, (b - a, 128), 0) == b - a - 1) & bottom, 0.0, grad1
                )
        lane = lanes((b - a, 128))
        grad2 = jnp.where(lane < 127, roll(value, 127), roll(bar_e[par, p + 2, a + 8 : b + 8], 127)) - value
        if p + 1 == TILES:
            grad2 = jnp.where((lane == 127) & right, 0.0, grad2)
        u1 = q1_v[par, p, a:b] + SIGMA * grad1
        u2 = q2_v[par, p, a:b] + SIGMA * grad2
        shrink = jnp.maximum(1.0, jnp.sqrt(u1 * u1 + u2 * u2) / WEIGHT)
        q1_v[par, p, a:b] = u1 / shrink
        q2_v[par, p, a:b] = u2 / shrink

    def moved_tiles(par, a, b, wanted):
        firsts = [roll(spread[par, 0, p, a:b], 113) if wanted(p - 1) or wanted(p) else None for p in range(TILES)]
        seconds = [roll(spread[par, 1, p, a:b], 49) if wanted(p) or wanted(p + 1) else None for p in range(TILES)]
        return firsts + [0.0], [0.0] + seconds

    def merged(p, tiles, rows_count):
        firsts, seconds = tiles
        lane = lanes((rows_count, 128))
        if p == -1:
            return jnp.where(lane >= 113, firsts[0], 0.0)
        if p == TILES:
            return jnp.where(lane < 15, seconds[TILES], 0.0)
        return jnp.where(lane < 113, firsts[p], firsts[p + 1]) + jnp.where(lane >= 49, seconds[p + 1], seconds[p])

    def own_part(par, p, a, b, tiles):
        lane = lanes((b - a, 128))
        sub = lax.broadcasted_iota(jnp.int32, (b - a, 128), 0)
        i, j = a - 8, b - 8
        m1, m2 = q1_v[par, p, i:j], q2_v[par, p, i:j]
        if par == 1:
            above = q1_v[0, p, i:j]
            if b == 72:
                m1 = jnp.where((sub == b - a - 1) & bottom, 0.0, m1)
        elif a == 8:
            above = jnp.concatenate([jnp.zeros((1, 128), F32), q1_v[1, p, : j - 1]], axis=0)
        else:
            above = q1_v[1, p, i - 1 : j - 1]
        outer = roll(q2_v[par, p - 1, i:j], 1) if p else 0.0
        before = jnp.where(lane == 0, outer, roll(m2, 1))
        if p + 1 == TILES:
            m2 = jnp.where((lane == 127) & right, 0.0, m2)
        return merged(p, tiles, b - a) - ((m1 - above) + (m2 - before))

    def rim_part(par, p, d, tiles):
        value = merged(p, tiles, 8)
        if d == 1 and par == 0:
            edge = jnp.concatenate([q1_v[1, p, PAIRS - 1 : PAIRS], jnp.zeros((7, 128), F32)], axis=0)
            value = value + edge
        return value

    def side_part(par, s, a, b, tiles):
        value = merged(TILES if s else -1, tiles, b - a)
        if s == 1 and 8 <= a < 72:
            edge = roll(q2_v[par, TILES - 1, a - 8 : b - 8], 1)
            value = value + jnp.where(lanes((b - a, 128)) == 0, edge, 0.0)
        return value

    def masked(direction, value):
        return jnp.where(outside[direction], 0.0, value)

    def duals(edge):
        gap = jnp.zeros((PAIRS - 2 * edge, 128), F32)

        def rows_full(p):
            return 0 if p == 0 else 1 if p + 1 == TILES else None

        def blur_halo(p):
            full = rows_full(p)
            ranges = [(full, 0, PAIRS)] if full is not None else []
            for h in (0, 1):
                if h != full:
                    ranges += [(h, 0, edge), (h, PAIRS - edge, edge)]
            return jnp.dot(
                stacked_rows(shifted_halo, p, ranges),
                weights[p * W_ROWS : p * W_ROWS + W_ROWS],
                preferred_element_type=F32,
            )

        def dual(p, extra):
            full = rows_full(p)
            halves, place_r = [None, None], 0
            if full is not None:
                halves[full] = blur_v[p, PAIRS * full : PAIRS * full + PAIRS] + extra[:PAIRS]
                place_r = PAIRS
            for h in (0, 1):
                if h != full:
                    more = jnp.concatenate(
                        [extra[place_r : place_r + edge], gap, extra[place_r + edge : place_r + 2 * edge]], axis=0
                    )
                    halves[h] = blur_v[p, PAIRS * h : PAIRS * h + PAIRS] + more
                    place_r += 2 * edge
            even = jnp.where(lane64 < 64, halves[0], roll(halves[1], 64))
            odd = jnp.where(lane64 < 64, roll(halves[0], 64), halves[1])
            new = []
            for par, value in ((0, even), (1, odd)):
                updated = (y_v[par, p] + SIGMA * (value - obs_v[par, p])) / (1.0 + SIGMA)
                y_v[par, p] = updated
                new.append(updated)
            ypad[0, p, 16 : 16 + PAIRS] = jnp.where(lane64 < 64, new[0], roll(new[1], 64))
            ypad[1, p, 16 : 16 + PAIRS] = jnp.where(lane64 < 64, roll(new[0], 64), new[1])

        def adjoint(p):
            out = jnp.dot(
                jnp.concatenate(
                    [
                        jnp.concatenate([ypad[h, p, 16 - t : 96 - t] for h in (0, 1)], axis=0).astype(BF16)
                        for t in range(16)
                    ],
                    axis=1,
                ),
                weights_t[p * T_ROWS : p * T_ROWS + 2048],
                preferred_element_type=F32,
            )
            for h in (0, 1):
                spread[1, h, p, 0:80] = out[80 * h : 80 * h + 80, 0:128]
                spread[0, h, p, 1:81] = out[80 * h : 80 * h + 80, 128:256]

        order = (0, 1, 3, 2)
        extras = {p: blur_halo(p) for p in order}
        for p in order:
            dual(p, extras[p])
        for p in order:
            adjoint(p)

    for par in (0, 1):
        lay(shifted, par, 8, 72)
    for p in range(TILES):
        blur_own(p, 0)
    for p in range(TILES - 1):
        tv(0, p, 0, PAIRS)
        tv(1, p, 0, PAIRS - 8)

    wait_in(0)
    for par in (0, 1):
        for d, (a, b) in ((0, (0, 8)), (1, (72, 80))):
            for p in range(TILES):
                value = masked(d, row_in[d, par, p])
                x_e[par, p + 1, a:b] = value
                bar_e[par, p + 1, a:b] = value
            for s, q in ((0, 0), (1, TILES + 1)):
                value = masked(4 + 2 * d + s, unpacked(cor_in[0, 2 * d + s], par, 112 - 112 * s))
                x_e[par, q, a:b] = value
                bar_e[par, q, a:b] = value
        for s, q in ((0, 0), (1, TILES + 1)):
            for k in range(4):
                value = masked(2 + s, unpacked(col_in[0, s], 4 * par + k, 112 - 112 * s))
                x_e[par, q, 8 + 16 * k : 24 + 16 * k] = value
                bar_e[par, q, 8 + 16 * k : 24 + 16 * k] = value
        lay(shifted_halo, par, 0, 8)
        lay(shifted_halo, par, 72, 80)
        lay_sides(par, 8, 72, 0)

    duals(8)
    for p in range(TILES - 1):
        tv(1, p, PAIRS - 8, PAIRS)
    for par in (0, 1):
        tv(par, TILES - 1, 0, PAIRS)

    every = lambda p: True
    for par in (0, 1):
        for d, first in ((0, 0), (1, 64)):
            strip = [[], [], [], []]
            for a, b in ((first, first + 8), (first + 8, first + 16)):
                own = 8 <= a < 72
                tiles = moved_tiles(par, a, b, every)
                for p in range(TILES):
                    value = own_part(par, p, a, b, tiles) if own else rim_part(par, p, d, tiles)
                    acc[par, p + 1, a:b] = value
                    strip[p].append(value)
                acc[par, 0, a:b] = side_part(par, 0, a, b, tiles)
                acc[par, TILES + 1, a:b] = side_part(par, 1, a, b, tiles)
            for p in range(TILES):
                wide_row_out[d, TILES * par + p] = jnp.concatenate(strip[p], axis=0).astype(STRIP_TYPE)
        a, b = 16, 64
        tiles = moved_tiles(par, a, b, lambda p: p not in (1, 2))
        for p in (0, TILES - 1):
            acc[par, p + 1, a:b] = own_part(par, p, a, b, tiles)
        acc[par, 0, a:b] = side_part(par, 0, a, b, tiles)
        acc[par, TILES + 1, a:b] = side_part(par, 1, a, b, tiles)
    for d, first in ((0, 0), (1, 64)):
        message = None
        for f, (par, s) in enumerate(((0, 0), (0, 1), (1, 0), (1, 1))):
            moved = roll(acc[par, (TILES + 1) * s, first : first + 16], 16 * f - 112 + 112 * s)
            message = moved if f == 0 else jnp.where(lane16 >= 16 * f, moved, message)
        wide_row_out[d, 2 * TILES] = message.astype(STRIP_TYPE)
    for s, q in ((0, 0), (1, TILES)):
        around = [
            jnp.where(lanes((80, 128)) < 16, roll(acc[par, q], 16), roll(acc[par, q + 1], 16)) for par in (0, 1)
        ]
        message = None
        for f in range(4):
            moved = roll(around[f >> 1][40 * (f & 1) : 40 * (f & 1) + 40], 32 * f)
            message = moved if f == 0 else jnp.where(lanes((40, 128)) >= 32 * f, moved, message)
        wide_col_out[s] = message
        for d, first in ((0, 0), (1, 64)):
            message = None
            for f in range(4):
                start = first + 8 * (f & 1)
                moved = roll(around[f >> 1][start : start + 8], 32 * f)
                message = moved if f == 0 else jnp.where(lane8 >= 32 * f, moved, message)
            wide_cor_out[2 * d + s] = message
    start_out(1)

    for par in (0, 1):
        a, b = 16, 64
        tiles = moved_tiles(par, a, b, lambda p: p in (1, 2))
        for p in range(TILES):
            value = own_part(par, p, a, b, tiles) if p in (1, 2) else acc[par, p + 1, a:b]
            old = x_e[par, p + 1, a:b]
            new = old - TAU * value
            x_e[par, p + 1, a:b] = new
            bar_e[par, p + 1, a:b] = 2.0 * new - old
        lay(shifted, par, a, b)
        lane = lanes((b - a, 128))
        for v in (0, 1):
            offset = starts_at(par, v)
            first, last = shifted[par, v, 0, 0, a:b], shifted[par, v, 1, TILES - 1, a:b]
            shifted[par, v, 0, 0, a:b] = jnp.where(beyond(lane, offset, 30), first, 0.0)
            shifted[par, v, 1, TILES - 1, a:b] = jnp.where(beyond(lane, offset, 64), 0.0, last)
            for h in (0, 1):
                for p in range(TILES):
                    shifted[par, v, h, p, 8:16] = jnp.zeros((8, 128), F32)
                    shifted[par, v, h, p, 64:72] = jnp.zeros((8, 128), F32)
    lax.fori_loop(0, TILES, blur_own, 0)
    for p in (1, 2):
        tv(0, p, 8, 56)
        tv(1, p, 8, 48)

    wait_in(1)
    strips = [[wide_row_in[d, i].astype(F32) for i in range(2 * TILES + 1)] for d in (0, 1)]
    for par in (0, 1):
        beside = []
        for s in (0, 1):
            halves = [masked(2 + s, wide_col_in[s]) for _ in (0, 1)]
            lane = lanes((40, 128))
            low = [jnp.where(lane >= 112, roll(halves[k], 112 - 32 * (2 * par + k)), 0.0) for k in (0, 1)]
            high = [jnp.where(lane < 16, roll(halves[k], -16 - 32 * (2 * par + k)), 0.0) for k in (0, 1)]
            beside.append((jnp.concatenate(low, axis=0), jnp.concatenate(high, axis=0)))
        for a, b in ((16, 64),):
            for s, q in ((0, 0), (1, TILES)):
                for k in (0, 1):
                    more = beside[s][k][a:b]
                    old = x_e[par, q + k, a:b]
                    if q + k in (0, TILES + 1):
                        value = acc[par, q + k, a:b] + more
                        new = old - TAU * value
                        bar_e[par, q + k, a:b] = masked(2 + s, 2.0 * new - old)
                    else:
                        x_e[par, q + k, a:b] = old - TAU * more
                        bar_e[par, q + k, a:b] = bar_e[par, q + k, a:b] - 2.0 * TAU * more
        for d, first in ((0, 0), (1, 64)):
            for k8 in (0, 1):
                a, b = first + 8 * k8, first + 8 * k8 + 8
                for q in range(TILES + 2):
                    value = acc[par, q, a:b]
                    if 1 <= q <= TILES:
                        value = value + masked(d, strips[d][TILES * par + q - 1][8 * k8 : 8 * k8 + 8])
                    else:
                        s = 0 if q == 0 else 1
                        f = 2 * par + s
                        more = roll(strips[d][2 * TILES][8 * k8 : 8 * k8 + 8], 112 - 112 * s - 16 * f)
                        value = value + masked(d, jnp.where((lane8 >= 112) if s == 0 else (lane8 < 16), more, 0.0))
                    for s, line in ((0, 0), (1, TILES)):
                        if q in (line, line + 1):
                            message = wide_cor_in[2 * d + s]
                            f = 2 * par + k8
                            if q == line:
                                more = jnp.where(lane8 >= 112, roll(message, 112 - 32 * f), 0.0)
                            else:
                                more = jnp.where(lane8 < 16, roll(message, -16 - 32 * f), 0.0)
                            value = value + beside[s][q - line][a:b] + masked(4 + 2 * d + s, more)
                    old = x_e[par, q, a:b]
                    new = old - TAU * value
                    bar = 2.0 * new - old
                    if q == 0:
                        bar = masked(2, bar)
                    if q == TILES + 1:
                        bar = masked(3, bar)
                    if not 8 <= a < 72:
                        bar = masked(d, bar)
                    x_e[par, q, a:b] = new
                    bar_e[par, q, a:b] = bar
        lay(shifted_halo, par, 0, 16)
        lay(shifted_halo, par, 64, 80)
        lay_sides(par, 16, 64, 15)

    duals(16)
    for p in (1, 2):
        tv(0, p, 0, 8)
        tv(0, p, 56, 64)
        tv(1, p, 0, 8)
        tv(1, p, 48, 64)
    for par in (0, 1):
        for p in (0, TILES - 1):
            tv(par, p, 0, PAIRS)

    corners = [[None, None] for _ in range(4)]
    strip = [[[], [], [], []] for _ in (0, 1)]
    for par in (0, 1):
        for d, (a, b) in ((0, (0, 8)), (1, (72, 80))):
            tiles = moved_tiles(par, a, b, every)
            for p in range(TILES):
                strip[d][p].append(rim_part(par, p, d, tiles))
            for s in (0, 1):
                corners[2 * d + s][par] = side_part(par, s, a, b, tiles)
    for d in (0, 1):
        for p in range(TILES):
            last_row_out[d, p] = jnp.concatenate(strip[d][p], axis=0)
    for s, first_lane in ((0, 112), (1, 0)):
        side = [
            side_part(par, s, 8, 72, moved_tiles(par, 8, 72, lambda p: p == (TILES if s else -1)))
            for par in (0, 1)
        ]
        col_out[1, s] = packed([side[par][16 * k : 16 * k + 16] for par in (0, 1) for k in range(4)], first_lane, 16)
        for d in (0, 1):
            cor_out[1, 2 * d + s] = packed(corners[2 * d + s], first_lane, 8)
    start_out(2)

    for par in (0, 1):
        tiles = moved_tiles(par, 8, 72, every)
        for p in range(TILES):
            x_e[par, p + 1, 8:72] = x_e[par, p + 1, 8:72] - TAU * own_part(par, p, 8, 72, tiles)
            dual_out_ref[p, pl.ds(par, PAIRS, stride=2), :] = y_v[par, p]

    wait_in(2)
    strips = [[last_row_in[d, p] for p in range(TILES)] for d in (0, 1)]

    def subtract(par, q, a, b, value):
        x_e[par, q, a:b] = x_e[par, q, a:b] - TAU * value

    for par in (0, 1):
        for s, q, first_lane in ((0, 1, 0), (1, TILES, 112)):
            message = masked(2 + s, col_in[1, s])
            keep = lane16 < 15 if s == 0 else lane16 >= 113
            for k in range(4):
                value = jnp.where(keep, unpacked(message, 4 * par + k, first_lane), 0.0)
                subtract(par, q, 8 + 16 * k, 24 + 16 * k, value)
        for d, (a, b) in ((0, (8, 16)), (1, (64, 72))):
            for p in range(TILES):
                value = masked(d, strips[d][p][8 * par : 8 * par + 8])
                if p in (0, TILES - 1):
                    s = 0 if p == 0 else 1
                    message = masked(4 + 2 * d + s, cor_in[1, 2 * d + s])
                    keep = lane8 < 15 if s == 0 else lane8 >= 113
                    value = value + jnp.where(keep, unpacked(message, par, 112 * s), 0.0)
                subtract(par, p + 1, a, b, value)
    for par in (0, 1):
        for p in range(TILES):
            restored_ref[p, pl.ds(par, PAIRS, stride=2), :] = x_e[par, p + 1, 8:72]
    for exchange in range(EXCHANGES):
        wait_out(exchange)


def put_out(restored_ref, dual_ref, restored_hbm, dual_hbm, store_sem):
    stores = [
        pltpu.make_async_copy(src.at[p], dst.at[:, 128 * p : 128 * p + 128], store_sem.at[TILES * i + p])
        for i, (src, dst) in enumerate(((restored_ref, restored_hbm), (dual_ref, dual_hbm)))
        for p in range(TILES)
    ]
    for store in stores:
        store.start()
    for store in stores:
        store.wait()


def per_device(observed, psf_table, psf_index, start_image, blur_dual, tv_dual):
    shape = observed.shape
    block = (2, TILES, PAIRS, 128)
    extended = (2, TILES + 2, 80, 128)
    tiled = (TILES, 2 * PAIRS, 128)
    hbm = pl.BlockSpec(memory_space=pl.ANY)
    table = psf_table.transpose(1, 2, 0)
    results = pl.pallas_call(
        kernel,
        out_shape=(pltpu.VMEM(tiled, F32), pltpu.VMEM(tiled, F32)),
        in_specs=[hbm] * 6,
        out_specs=(pl.BlockSpec(memory_space=pltpu.VMEM),) * 2,
        scratch_shapes=[
            pltpu.VMEM(tiled, F32),
            pltpu.VMEM(table.shape, BF16),
            pltpu.SMEM(psf_index.shape, jnp.int32),
            pltpu.VMEM(tiled, F32),
            pltpu.VMEM(tiled, F32),
            pltpu.VMEM((2,) + tiled, F32),
            pltpu.VMEM((8, 64, 128), F32),
            pltpu.VMEM((TILES * W_ROWS, 128), BF16),
            pltpu.VMEM((TILES * T_ROWS, 256), BF16),
            pltpu.VMEM(extended, F32),
            pltpu.VMEM(extended, F32),
            pltpu.VMEM(extended, F32),
            pltpu.VMEM(block, F32),
            pltpu.VMEM(block, F32),
            pltpu.VMEM(block, F32),
            pltpu.VMEM(block, F32),
            pltpu.VMEM((2, 2, 2, TILES, 80, 128), F32),
            pltpu.VMEM((2, 2, 2, TILES, 80, 128), F32),
            pltpu.VMEM((TILES, 128, 128), F32),
            pltpu.VMEM((2, TILES, 96, 128), F32),
            pltpu.VMEM((2, 2, TILES, 88, 128), F32),
            pltpu.VMEM((2, 2, TILES, 8, 128), F32),
            pltpu.VMEM((2, 2, 16, 128), F32),
            pltpu.VMEM((2, 4, 8, 128), F32),
            pltpu.VMEM((2, 2, TILES, 8, 128), F32),
            pltpu.VMEM((2, 2, 16, 128), F32),
            pltpu.VMEM((2, 4, 8, 128), F32),
            pltpu.VMEM((2, 2 * TILES + 1, 16, 128), STRIP_TYPE),
            pltpu.VMEM((2, 40, 128), F32),
            pltpu.VMEM((4, 8, 128), F32),
            pltpu.VMEM((2, 2 * TILES + 1, 16, 128), STRIP_TYPE),
            pltpu.VMEM((2, 40, 128), F32),
            pltpu.VMEM((4, 8, 128), F32),
            pltpu.VMEM((2, TILES, 16, 128), F32),
            pltpu.VMEM((2, TILES, 16, 128), F32),
            pltpu.SemaphoreType.DMA((4 * TILES + 2,)),
            pltpu.SemaphoreType.DMA((EXCHANGES, 8)),
            pltpu.SemaphoreType.DMA((EXCHANGES, 8)),
        ],
        compiler_params=pltpu.CompilerParams(collective_id=0, has_side_effects=True),
    )(psf_index, observed, table, start_image, blur_dual, tv_dual)
    return pl.pallas_call(
        put_out,
        out_shape=(jax.ShapeDtypeStruct(shape, F32), jax.ShapeDtypeStruct(shape, F32)),
        in_specs=[hbm] * 2,
        out_specs=(hbm, hbm),
        scratch_shapes=[pltpu.SemaphoreType.DMA((2 * TILES,))],
    )(*(pltpu.with_memory_space_constraint(result, pltpu.VMEM) for result in results))


def solution(mesh):
    placed = (
        P("row", "col"),
        P(),
        P("row", "col"),
        P("row", "col"),
        P("row", "col"),
        P(None, "row", "col"),
    )
    return jax.shard_map(
        per_device,
        mesh=mesh,
        in_specs=placed,
        out_specs=(P("row", "col"), P("row", "col")),
        check_vma=False,
    )
```
